32 devices in a mesh: dp: 8 (over z, y), tensor: 4 (over x, core).
Axes of the slice: x: 2, y: 2, z: 4, core: 2. Of those that a mesh axis runs over, the one named last changes fastest.
Arguments:
- clean_latents: bfloat16 [8, 512, 2048], P('dp', 'tensor'), may hold values from -24 to 24
- noise_latents: bfloat16 [8, 512, 2048], P('dp', 'tensor'), may hold values from -24 to 24
- step_index: int32 [8], P('dp'), may hold values from 0 to 999
- labels: int32 [8], P('dp'), may hold values from 0 to 999
- class_shift: bfloat16 [1000, 2048], replicated, may hold values from -6 to 6
- w_qkv: bfloat16 [2048, 3072], P('dp', 'tensor'), may hold values from -0.2 to 0.2
- w_out_t: bfloat16 [2048, 1024], P('dp', 'tensor'), may hold values from -0.1875 to 0.1875
Outputs:
- grad_qkv: float32 [2048, 3072], P('dp', 'tensor')
- grad_out: float32 [2048, 1024], P('dp', 'tensor')
The draws below stay inside these ranges and needn't reach their ends.
All inputs are finite; a program needn't handle non-finite values.
Results may differ from the reference program's by a relative error of at most 0.0075.
Values may be sent and summed in bfloat16 or wider, within the bound.
A program may use at most 128 MiB of HBM per device.

```python
import math
import jax
import jax.numpy as jnp
from jax import lax

D = 2048
HEADS = 8
HEAD_DIM = 128
CLASSES = 1000
STEPS = 1000
S = 512
LATENTS = 8


weight_edge = 0.19921875


def latent_draw(key, tag):
    folded = jax.random.fold_in(key, tag)
    key_base, key_rough = jax.random.split(folded, 2)
    full_shape = (LATENTS, S, D)
    rising = 0.5 + jnp.arange(S, dtype=jnp.float32) / S
    roughness = jnp.exp(jax.random.uniform(key_rough, (LATENTS, S, 1), jnp.float32, -0.7, 0.7))
    values = jax.random.normal(key_base, full_shape, jnp.float32) * rising[None, :, None] * roughness
    return jnp.clip(values, -24.0, 24.0).astype(jnp.bfloat16)


def draw_clean_latents(key, part):
    return latent_draw(key, 11)


def draw_noise_latents(key, part):
    return latent_draw(key, 23)


def draw_w_qkv(key, part):
    key_base = jax.random.fold_in(jax.random.fold_in(key, 37), 0)
    full_shape = (D, HEADS, 3, HEAD_DIM)
    values = jax.random.normal(key_base, full_shape, jnp.float32) / math.sqrt(D)
    return jnp.clip(values, -weight_edge, weight_edge).reshape(D, HEADS * 3 * HEAD_DIM).astype(jnp.bfloat16)


def touch_ends(array, own_key, smallest, high):
    longest = array.shape.index(max(array.shape))
    spots = []
    for shift in (0, 1):
        where = [jax.random.randint(jax.random.fold_in(own_key, axis), (), 0, length) for axis, length in enumerate(array.shape)]
        where[longest] = (where[longest] + shift) % array.shape[longest]
        spots.append(tuple(where))
    return array.at[spots[0]].set(smallest).at[spots[1]].set(high)


def block_scale(rng, dims, shards, low, high):
    def one(axis_at, shards_of):
        draws = jax.random.uniform(jax.random.fold_in(jax.random.fold_in(rng, 6), axis_at), (shards_of,), jnp.float32, low / len(shards), high / len(shards))
        return jnp.repeat(jnp.exp(draws), dims[axis_at] // shards_of).reshape((-1,) + (1,) * (len(dims) - axis_at - 1))

    level = one(*shards[0])
    for cut in shards[1:]:
        level = level * one(*cut)
    return level


def bell_draw(own_key, shape, width, limit, pieces=(), kind=jnp.bfloat16):
    loudness = block_scale(own_key, shape, pieces, -0.22, 0.18) if pieces else 1.0
    entries = jax.random.normal(own_key, shape, jnp.float32) * width * loudness
    return jnp.minimum(jnp.maximum(entries, -limit), limit).astype(kind)


def setup_inputs(seed: int = 0) -> dict:
    streams_of = jax.random.split(jax.random.key(seed), 8)
    return {
        "clean_latents": draw_clean_latents(jax.random.fold_in(streams_of[7], 71), 0),
        "noise_latents": draw_noise_latents(jax.random.fold_in(streams_of[7], 71), 0),
        "step_index": touch_ends(jax.random.randint(streams_of[2], (LATENTS,), 0, STEPS), jax.random.fold_in(streams_of[2], 1), 0, STEPS - 1).astype(jnp.int32),
        "labels": touch_ends(jax.random.randint(streams_of[3], (LATENTS,), 0, CLASSES), jax.random.fold_in(streams_of[3], 1), 0, CLASSES - 1).astype(jnp.int32),
        "class_shift": bell_draw(streams_of[4], (CLASSES, D), 1.0, 6.0),
        "w_qkv": draw_w_qkv(jax.random.fold_in(streams_of[7], 71), 0),
        "w_out_t": bell_draw(streams_of[6], (D, HEADS * HEAD_DIM), (HEADS * HEAD_DIM) ** -0.5, 0.1875, ((0, 8), (1, 4))),
    }


norm_eps = 1e-06
target_floor = 0.1

def time_terms(step_index, model_width):
    step_times = 1.4 * (step_index.astype(jnp.float32) + 0.5) / STEPS
    feature_ids = jnp.arange(model_width, dtype=jnp.float32)
    frequency = jnp.exp(-math.log(100.0) * feature_ids / model_width)
    phases = step_times[:, None] * frequency[None, :] + feature_ids[None, :]
    return (step_times, 0.5 * jnp.sin(phases), 0.5 * frequency[None, :] * jnp.cos(phases))

def trig_path(clean_part, noise_part, step_times):
    cos_t = jnp.cos(step_times)[:, None, None]
    sin_t = jnp.sin(step_times)[:, None, None]
    clean_wide = clean_part.astype(jnp.float32)
    noise_wide = noise_part.astype(jnp.float32)
    return (cos_t * clean_wide + sin_t * noise_wide, cos_t * noise_wide - sin_t * clean_wide)

def modulate(noisy, velocity, amplitude, amp_rate, class_offset):
    inverse = lax.rsqrt(lax.optimization_barrier(jnp.mean(noisy * noisy, axis=-1, keepdims=True)) + norm_eps)
    normed = noisy * inverse
    normed_rate = velocity * inverse - noisy * inverse ** 3 * lax.optimization_barrier(jnp.mean(noisy * velocity, axis=-1, keepdims=True))
    scale_up = 1.0 + amplitude[:, None, :]
    mixed = normed * scale_up + class_offset[:, None, :]
    mixed_rate = normed_rate * scale_up + normed * amp_rate[:, None, :]
    return (mixed.astype(jnp.bfloat16), mixed_rate.astype(jnp.bfloat16))

def target_of(noisy, velocity, proj, proj_rate, step_times):
    cos_t = jnp.cos(step_times)[:, None, None]
    sin_t = jnp.sin(step_times)[:, None, None]
    model_out = noisy + proj
    model_rate = velocity + proj_rate
    return -(cos_t * cos_t) * (model_out - velocity) - cos_t * sin_t * (noisy + model_rate)

def wide_einsum(form, left_part, right_part):
    return jnp.einsum(form, left_part.astype(jnp.float32), right_part.astype(jnp.float32))

def attend(projected, projected_rate, score_scale):
    query_part = projected[:, :, :, 0, :]
    key_part = projected[:, :, :, 1, :]
    value_part = projected[:, :, :, 2, :]
    query_rate = projected_rate[:, :, :, 0, :]
    key_rate = projected_rate[:, :, :, 1, :]
    value_rate = projected_rate[:, :, :, 2, :]
    scores = wide_einsum('lqhd,lkhd->lhqk', query_part, key_part) * score_scale
    score_rate = (wide_einsum('lqhd,lkhd->lhqk', query_rate, key_part) + wide_einsum('lqhd,lkhd->lhqk', query_part, key_rate)) * score_scale
    attn_probs = jax.nn.softmax(scores, axis=-1)
    probs_low = attn_probs.astype(jnp.bfloat16)
    prob_rate = attn_probs * (score_rate - lax.optimization_barrier(jnp.sum(attn_probs * score_rate, axis=-1, keepdims=True)))
    prob_rate_low = prob_rate.astype(jnp.bfloat16)
    attn_out = wide_einsum('lhqk,lkhd->lqhd', probs_low, value_part)
    attn_rate = wide_einsum('lhqk,lkhd->lqhd', prob_rate_low, value_part) + wide_einsum('lhqk,lkhd->lqhd', probs_low, value_rate)
    return (attn_probs, probs_low, attn_out.astype(jnp.bfloat16), attn_rate.astype(jnp.bfloat16))

def attend_back(attn_grad, attn_probs, probs_low, projected, score_scale):
    query_part = projected[:, :, :, 0, :]
    key_part = projected[:, :, :, 1, :]
    value_part = projected[:, :, :, 2, :]
    prob_grad = wide_einsum('lqhd,lkhd->lhqk', attn_grad, value_part)
    value_grad = wide_einsum('lhqk,lqhd->lkhd', probs_low, attn_grad)
    score_grad = (attn_probs * (prob_grad - lax.optimization_barrier(jnp.sum(attn_probs * prob_grad, axis=-1, keepdims=True))) * score_scale).astype(jnp.bfloat16)
    query_grad = wide_einsum('lhqk,lkhd->lqhd', score_grad, key_part)
    key_grad = wide_einsum('lhqk,lqhd->lkhd', score_grad, query_part)
    return jnp.stack([query_grad, key_grad, value_grad], axis=3).astype(jnp.bfloat16)

def reference(clean_latents, noise_latents, step_index, labels, class_shift, w_qkv, w_out_t):
    loss_scale = 1.0 / math.sqrt(LATENTS * S)
    score_scale = 1.0 / math.sqrt(HEAD_DIM)
    step_times, amplitude, amp_rate = time_terms(step_index, D)
    class_offset = class_shift[labels].astype(jnp.float32)

    def per_latent(totals, inputs_one):
        grad_in_sum, grad_out_sum = totals
        clean_one, noise_one, time_one, amp_one, rate_one, offset_one = inputs_one
        noisy, velocity = trig_path(clean_one[None], noise_one[None], time_one[None])
        mixed, mixed_rate = modulate(noisy, velocity, amp_one[None], rate_one[None], offset_one[None])
        mixed_rows = mixed.reshape(S, D)
        rate_rows = mixed_rate.reshape(S, D)
        projected = jnp.dot(mixed_rows, w_qkv, preferred_element_type=jnp.float32).astype(jnp.bfloat16).reshape(1, S, HEADS, 3, HEAD_DIM)
        projected_rate = jnp.dot(rate_rows, w_qkv, preferred_element_type=jnp.float32).astype(jnp.bfloat16).reshape(1, S, HEADS, 3, HEAD_DIM)
        attn_probs, probs_low, attn_out, attn_rate = attend(projected, projected_rate, score_scale)
        attn_rows = attn_out.reshape(S, HEADS * HEAD_DIM)
        attn_rate_rows = attn_rate.reshape(S, HEADS * HEAD_DIM)
        proj = jnp.dot(attn_rows, w_out_t.T, preferred_element_type=jnp.float32).reshape(1, S, D)
        proj_rate = jnp.dot(attn_rate_rows, w_out_t.T, preferred_element_type=jnp.float32).reshape(1, S, D)
        target = target_of(noisy, velocity, proj, proj_rate, time_one[None])
        spread = jnp.sqrt(jnp.mean(target * target))
        cotangent = (-(target / (spread + target_floor)) * loss_scale).astype(jnp.bfloat16).reshape(S, D)
        grad_out_sum = grad_out_sum + jnp.dot(cotangent.T, attn_rows, preferred_element_type=jnp.float32)
        attn_grad = jnp.dot(cotangent, w_out_t, preferred_element_type=jnp.float32).astype(jnp.bfloat16).reshape(1, S, HEADS, HEAD_DIM)
        qkv_grad = attend_back(attn_grad, attn_probs, probs_low, projected, score_scale).reshape(S, HEADS * 3 * HEAD_DIM)
        grad_in_sum = grad_in_sum + jnp.dot(mixed_rows.T, qkv_grad, preferred_element_type=jnp.float32)
        return ((grad_in_sum, grad_out_sum), None)
    zero_grads = (jnp.zeros((D, HEADS * 3 * HEAD_DIM), jnp.float32), jnp.zeros((D, HEADS * HEAD_DIM), jnp.float32))
    (grad_qkv, grad_out), _ = lax.scan(per_latent, zero_grads, (clean_latents, noise_latents, step_times, amplitude, amp_rate, class_offset))
    return (grad_qkv, grad_out)
```

```python
import functools
import math

import jax
import jax.numpy as jnp
from jax import lax
from jax.experimental import pallas as pl
from jax.experimental.pallas import tpu as pltpu
from jax.sharding import PartitionSpec as P

HEAD_DIM = 128
STEPS = 1000


norm_eps = 1e-06
target_floor = 0.1


def time_terms(step_index, model_width):
    step_times = 1.4 * (step_index.astype(jnp.float32) + 0.5) / STEPS
    feature_ids = jnp.arange(model_width, dtype=jnp.float32)
    frequency = jnp.exp(-math.log(100.0) * feature_ids / model_width)
    phases = step_times[:, None] * frequency[None, :] + feature_ids[None, :]
    return (step_times, 0.5 * jnp.sin(phases), 0.5 * frequency[None, :] * jnp.cos(phases))


def low_einsum(form, left_part, right_part):
    return jnp.einsum(form, left_part, right_part, preferred_element_type=jnp.float32)


def attend(projected, projected_rate, score_scale):
    query_part = projected[:, :, :, 0, :]
    key_part = projected[:, :, :, 1, :]
    value_part = projected[:, :, :, 2, :]
    query_rate = projected_rate[:, :, :, 0, :]
    key_rate = projected_rate[:, :, :, 1, :]
    value_rate = projected_rate[:, :, :, 2, :]
    scores = low_einsum("lqhd,lkhd->lhqk", query_part, key_part) * score_scale
    score_rate = (
        low_einsum("lqhd,lkhd->lhqk", query_rate, key_part)
        + low_einsum("lqhd,lkhd->lhqk", query_part, key_rate)
    ) * score_scale
    attn_probs = jax.nn.softmax(scores, axis=-1)
    probs_low = attn_probs.astype(jnp.bfloat16)
    prob_rate = attn_probs * (score_rate - jnp.sum(attn_probs * score_rate, axis=-1, keepdims=True))
    prob_rate_low = prob_rate.astype(jnp.bfloat16)
    attn_out = low_einsum("lhqk,lkhd->lqhd", probs_low, value_part)
    attn_rate = low_einsum("lhqk,lkhd->lqhd", prob_rate_low, value_part) + low_einsum(
        "lhqk,lkhd->lqhd", probs_low, value_rate
    )
    return (attn_probs, probs_low, attn_out, attn_rate)


def attend_back(attn_grad, attn_probs, probs_low, projected, score_scale):
    query_part = projected[:, :, :, 0, :]
    key_part = projected[:, :, :, 1, :]
    value_part = projected[:, :, :, 2, :]
    prob_grad = low_einsum("lqhd,lkhd->lhqk", attn_grad, value_part)
    value_grad = low_einsum("lhqk,lqhd->lkhd", probs_low, attn_grad)
    score_grad = (
        attn_probs
        * (prob_grad - jnp.sum(attn_probs * prob_grad, axis=-1, keepdims=True))
        * score_scale
    ).astype(jnp.bfloat16)
    query_grad = low_einsum("lhqk,lkhd->lqhd", score_grad, key_part)
    key_grad = low_einsum("lhqk,lqhd->lkhd", score_grad, query_part)
    return jnp.stack([query_grad, key_grad, value_grad], axis=3).astype(jnp.bfloat16)


def row_contract(left_part, right_part):
    return lax.dot_general(
        left_part, right_part, (((0,), (0,)), ((), ())), preferred_element_type=jnp.float32
    )


MESH = pl.DeviceIdType.MESH
VMEM = pl.BlockSpec(memory_space=pltpu.VMEM)
HBM = pl.BlockSpec(memory_space=pl.ANY)


def places():
    dp_here, tensor_here = lax.axis_index("dp"), lax.axis_index("tensor")
    sibling = tensor_here + 1 - 2 * lax.rem(tensor_here, 2)
    opposite = lax.rem(tensor_here + 2, 4)
    diagonal = lax.rem(sibling + 2, 4)
    return dp_here, tensor_here, sibling, opposite, diagonal


def greet(devices):
    barrier = pltpu.get_barrier_semaphore()
    for device in devices:
        pl.semaphore_signal(barrier, inc=1, device_id=device, device_id_type=MESH)
    pl.semaphore_wait(barrier, len(devices))


def remote(source, target, send_sem, recv_sem, device):
    return pltpu.make_async_remote_copy(
        src_ref=source,
        dst_ref=target,
        send_sem=send_sem,
        recv_sem=recv_sem,
        device_id=device,
        device_id_type=MESH,
    )


def rows_of(ref, index, count):
    return ref.at[pl.ds(pl.multiple_of(index * count, count), count)]


def gather_kernel(
    dp_size, clean, noise, aux, w_qkv, w_out, mixed_all, rate_all, qkv_all, out_all,
    mixed, rate, w_send, w_recv, t_send, t_recv, own_sem,
):
    dp_here, tensor_here, sibling, opposite, diagonal = places()
    part = clean.shape[0]
    qkv_rows = w_qkv.shape[0]
    peers = [(lax.rem(dp_here + step, dp_size), tensor_here) for step in range(1, dp_size)]
    greet(peers + [(dp_here, sibling), (dp_here, opposite)])
    weight_copies = []
    for which, (held, full) in enumerate(((w_qkv, qkv_all), (w_out, out_all))):
        for step, peer in enumerate(peers):
            copy = remote(
                held, rows_of(full, dp_here, qkv_rows), w_send.at[which, step], w_recv.at[which, step], peer
            )
            copy.start()
            weight_copies.append(copy)
    local_copies = [
        pltpu.make_async_copy(w_qkv, rows_of(qkv_all, dp_here, qkv_rows), own_sem.at[0]),
        pltpu.make_async_copy(w_out, rows_of(out_all, dp_here, qkv_rows), own_sem.at[1]),
    ]
    for copy in local_copies:
        copy.start()
    cos_t, sin_t = aux[3:4, :], aux[4:5, :]
    scale_up, amp_rate, offset = aux[0:1, :], aux[1:2, :], aux[2:3, :]

    @pl.loop(0, part // 16)
    def _(index):
        rows = pl.ds(pl.multiple_of(index * 16, 16), 16)
        clean_wide = clean[rows, :].astype(jnp.float32)
        noise_wide = noise[rows, :].astype(jnp.float32)
        noisy = cos_t * clean_wide + sin_t * noise_wide
        velocity = cos_t * noise_wide - sin_t * clean_wide
        inverse = lax.rsqrt(jnp.mean(noisy * noisy, axis=-1, keepdims=True) + norm_eps)
        cross = jnp.mean(noisy * velocity, axis=-1, keepdims=True)
        normed = noisy * inverse
        normed_rate = velocity * inverse - noisy * (inverse * inverse * inverse * cross)
        mixed[rows, :] = (normed * scale_up + offset).astype(jnp.bfloat16)
        rate[rows, :] = (normed_rate * scale_up + normed * amp_rate).astype(jnp.bfloat16)

    sends, forwards = [], []
    for which, (held, full) in enumerate(((mixed, mixed_all), (rate, rate_all))):
        spot = rows_of(full, tensor_here, part)
        to_opposite = remote(held, spot, t_send.at[which, 0], t_recv.at[which, 0], (dp_here, opposite))
        to_opposite.start()
        to_sibling = remote(held, spot, t_send.at[which, 1], t_recv.at[which, 1], (dp_here, sibling))
        to_sibling.start()
        own = pltpu.make_async_copy(held, spot, own_sem.at[2 + which])
        own.start()
        local_copies.append(own)
        arrived = rows_of(full, opposite, part)
        forward = remote(arrived, arrived, t_send.at[which, 2], t_recv.at[which, 2], (dp_here, sibling))
        sends.append((to_opposite, to_sibling))
        forwards.append(forward)
    for (to_opposite, _), forward in zip(sends, forwards):
        to_opposite.wait_recv()
        forward.start()
    for (to_opposite, to_sibling), forward in zip(sends, forwards):
        to_opposite.wait_send()
        to_sibling.wait()
        forward.wait()
    for copy in weight_copies:
        copy.wait()
    for copy in local_copies:
        copy.wait()


def gather_all(dp_size, clean, noise, aux, w_qkv, w_out):
    part, width = clean.shape
    low = jnp.bfloat16
    return pl.pallas_call(
        functools.partial(gather_kernel, dp_size),
        out_shape=(
            jax.ShapeDtypeStruct((4 * part, width), low),
            jax.ShapeDtypeStruct((4 * part, width), low),
            jax.ShapeDtypeStruct((dp_size * w_qkv.shape[0], w_qkv.shape[1]), low),
            jax.ShapeDtypeStruct((dp_size * w_out.shape[0], w_out.shape[1]), low),
        ),
        in_specs=[VMEM] * 5,
        out_specs=(HBM,) * 4,
        scratch_shapes=[
            pltpu.VMEM((part, width), low),
            pltpu.VMEM((part, width), low),
            pltpu.SemaphoreType.DMA((2, dp_size)),
            pltpu.SemaphoreType.DMA((2, dp_size)),
            pltpu.SemaphoreType.DMA((2, 3)),
            pltpu.SemaphoreType.DMA((2, 3)),
            pltpu.SemaphoreType.DMA((4,)),
        ],
        compiler_params=pltpu.CompilerParams(
            collective_id=0, has_side_effects=True, vmem_limit_bytes=32 * 2**20
        ),
    )(clean, noise, aux, w_qkv, w_out)


PIECES = 4


def target_kernel(
    clean, noise, aux, partial, target_all, first, from_sibling, from_opposite, summed, target,
    load_sem, r_send, r_recv, g_send, g_recv,
):
    dp_here, tensor_here, sibling, opposite, diagonal = places()
    part = clean.shape[0]
    piece = part // PIECES
    greet([(dp_here, sibling), (dp_here, opposite)])

    def block(owner, index):
        return rows_of(partial, owner * PIECES + index, piece)

    def slot(ref, index):
        return ref.at[pl.ds(index * piece, piece)]

    cross, direct, across, loads = [], [], [], []
    for index in range(PIECES):
        copy = remote(
            block(diagonal, index), slot(from_sibling.at[0], index), r_send.at[0, index], r_recv.at[0, index],
            (dp_here, sibling),
        )
        copy.start()
        cross.append(copy)
        load = pltpu.make_async_copy(block(opposite, index), slot(first.at[0], index), load_sem.at[0, index])
        load.start()
        loads.append(load)
    own_loads = []
    for index in range(PIECES):
        copy = remote(
            block(sibling, index), slot(from_sibling.at[1], index), r_send.at[1, index], r_recv.at[1, index],
            (dp_here, sibling),
        )
        copy.start()
        direct.append(copy)
        load = pltpu.make_async_copy(block(tensor_here, index), slot(first.at[1], index), load_sem.at[1, index])
        load.start()
        own_loads.append(load)
    for index in range(PIECES):
        cross[index].wait_recv()
        loads[index].wait()
        rows = pl.ds(index * piece, piece)
        total = first[0, rows, :].astype(jnp.float32) + from_sibling[0, rows, :].astype(jnp.float32)
        summed[rows, :] = total.astype(jnp.bfloat16)
        copy = remote(
            slot(summed, index), slot(from_opposite, index), r_send.at[2, index], r_recv.at[2, index],
            (dp_here, opposite),
        )
        copy.start()
        across.append(copy)
    cos_t, sin_t = aux[3:4, :], aux[4:5, :]
    sends, forwards = [], []

    def spot(owner, index):
        return rows_of(target_all, owner * PIECES + index, piece)

    for index in range(PIECES):
        across[index].wait_recv()
        direct[index].wait_recv()
        own_loads[index].wait()
        rows = pl.ds(index * piece, piece)
        clean_wide = clean[rows, :].astype(jnp.float32)
        noise_wide = noise[rows, :].astype(jnp.float32)
        noisy = cos_t * clean_wide + sin_t * noise_wide
        velocity = cos_t * noise_wide - sin_t * clean_wide
        moved = (
            first[1, rows, :].astype(jnp.float32)
            + from_sibling[1, rows, :].astype(jnp.float32)
            + from_opposite[rows, :].astype(jnp.float32)
        )
        value = -(cos_t * cos_t) * (noisy - velocity) - cos_t * sin_t * (noisy + velocity) - moved
        target[rows, :] = value.astype(jnp.bfloat16)
        held = slot(target, index)
        to_opposite = remote(
            held, spot(tensor_here, index), g_send.at[0, index], g_recv.at[0, index], (dp_here, opposite)
        )
        to_opposite.start()
        to_sibling = remote(
            held, spot(tensor_here, index), g_send.at[1, index], g_recv.at[1, index], (dp_here, sibling)
        )
        to_sibling.start()
        own = pltpu.make_async_copy(held, spot(tensor_here, index), load_sem.at[2, index])
        own.start()
        forward = remote(
            spot(opposite, index), spot(opposite, index), g_send.at[2, index], g_recv.at[2, index], (dp_here, sibling)
        )
        sends.append((to_opposite, to_sibling, own, forward))
    for to_opposite, to_sibling, own, forward in sends:
        to_opposite.wait_recv()
        forward.start()
    for index, (to_opposite, to_sibling, own, forward) in enumerate(sends):
        to_opposite.wait_send()
        to_sibling.wait()
        own.wait()
        forward.wait()
        cross[index].wait_send()
        direct[index].wait_send()
        across[index].wait_send()


def gather_target(clean, noise, aux, partial):
    part, width = clean.shape
    low = jnp.bfloat16
    return pl.pallas_call(
        target_kernel,
        out_shape=jax.ShapeDtypeStruct((4 * part, width), low),
        in_specs=[VMEM, VMEM, VMEM, HBM],
        out_specs=HBM,
        scratch_shapes=[
            pltpu.VMEM((2, part, width), low),
            pltpu.VMEM((2, part, width), low),
            pltpu.VMEM((part, width), low),
            pltpu.VMEM((part, width), low),
            pltpu.VMEM((part, width), low),
            pltpu.SemaphoreType.DMA((3, PIECES)),
            pltpu.SemaphoreType.DMA((3, PIECES)),
            pltpu.SemaphoreType.DMA((3, PIECES)),
            pltpu.SemaphoreType.DMA((3, PIECES)),
            pltpu.SemaphoreType.DMA((3, PIECES)),
        ],
        compiler_params=pltpu.CompilerParams(
            collective_id=1, has_side_effects=True, vmem_limit_bytes=32 * 2**20
        ),
    )(clean, noise, aux, partial)


def scatter_kernel(
    dp_size, in_partial, out_partial, in_sum, out_sum, in_slots, out_slots, send_sem, recv_sem, own_sem
):
    dp_here, tensor_here, _, _, _ = places()
    rows = in_sum.shape[0]
    peers = [(lax.rem(dp_here + step, dp_size), tensor_here) for step in range(1, dp_size)]
    greet(peers)
    pairs = ((in_partial, in_slots, in_sum), (out_partial, out_slots, out_sum))
    copies, own_copies = [], []
    for which, (source, slots, _) in enumerate(pairs):
        row = []
        for step, peer in enumerate(peers):
            copy = remote(
                rows_of(source, peer[0], rows), slots.at[step + 1], send_sem.at[which, step],
                recv_sem.at[which, step], peer,
            )
            copy.start()
            row.append(copy)
        copies.append(row)
        own = pltpu.make_async_copy(rows_of(source, dp_here, rows), slots.at[0], own_sem.at[which])
        own.start()
        own_copies.append(own)
    tile = min(rows, 32)
    for which, (_, slots, total) in enumerate(pairs):
        own_copies[which].wait()
        for copy in copies[which]:
            copy.wait_recv()

        @pl.loop(0, rows // tile)
        def _(index):
            spot = pl.ds(pl.multiple_of(index * tile, tile), tile)
            value = slots[0, spot, :].astype(jnp.float32)
            value = lax.fori_loop(
                1, dp_size, lambda step, held: held + slots[step, spot, :].astype(jnp.float32), value
            )
            total[spot, :] = value

    for row in copies:
        for copy in row:
            copy.wait_send()


def scatter_all(dp_size, in_partial, out_partial):
    rows = in_partial.shape[0] // dp_size
    in_cols, out_cols = in_partial.shape[1], out_partial.shape[1]
    low = jnp.bfloat16
    return pl.pallas_call(
        functools.partial(scatter_kernel, dp_size),
        out_shape=(
            jax.ShapeDtypeStruct((rows, in_cols), jnp.float32),
            jax.ShapeDtypeStruct((rows, out_cols), jnp.float32),
        ),
        in_specs=[HBM, HBM],
        out_specs=(VMEM, VMEM),
        scratch_shapes=[
            pltpu.VMEM((dp_size, rows, in_cols), low),
            pltpu.VMEM((dp_size, rows, out_cols), low),
            pltpu.SemaphoreType.DMA((2, dp_size)),
            pltpu.SemaphoreType.DMA((2, dp_size)),
            pltpu.SemaphoreType.DMA((2,)),
        ],
        compiler_params=pltpu.CompilerParams(
            collective_id=2, has_side_effects=True, vmem_limit_bytes=32 * 2**20
        ),
    )(in_partial, out_partial)


def local(dp_size, clean_latents, noise_latents, step_index, labels, class_shift, w_qkv, w_out_t):
    latent_count, part_len, model_width = clean_latents.shape
    head_cols = w_out_t.shape[1]
    heads_here = head_cols // HEAD_DIM
    score_scale = 1.0 / math.sqrt(HEAD_DIM)
    seq_len = part_len * 4
    loss_scale = 1.0 / math.sqrt(dp_size * latent_count * seq_len)
    step_times, amplitude, amp_rate = time_terms(step_index, model_width)
    offset = lax.dynamic_slice(class_shift, (labels[0], 0), (1, model_width)).astype(jnp.float32)
    cos_t, sin_t = jnp.cos(step_times[0]), jnp.sin(step_times[0])
    row = (1, model_width)
    aux = jnp.concatenate(
        [
            1.0 + amplitude,
            amp_rate,
            offset,
            jnp.broadcast_to(cos_t, row),
            jnp.broadcast_to(sin_t, row),
            jnp.zeros((3, model_width), jnp.float32),
        ]
    )
    clean, noise = clean_latents[0], noise_latents[0]
    mixed_rows, rate_rows, qkv_all, out_all = gather_all(dp_size, clean, noise, aux, w_qkv, w_out_t)
    heads_shape = (1, seq_len, heads_here, 3, HEAD_DIM)
    projected = jnp.dot(mixed_rows, qkv_all, preferred_element_type=jnp.float32)
    projected_rate = jnp.dot(rate_rows, qkv_all, preferred_element_type=jnp.float32)
    projected = projected.astype(jnp.bfloat16).reshape(heads_shape)
    projected_rate = projected_rate.astype(jnp.bfloat16).reshape(heads_shape)
    attn_probs, probs_low, attn_out, attn_rate = attend(projected, projected_rate, score_scale)
    attn_rows = attn_out.astype(jnp.bfloat16).reshape(seq_len, head_cols)
    blend = (cos_t * cos_t * attn_out + cos_t * sin_t * attn_rate).astype(jnp.bfloat16)
    partial = lax.dot_general(
        blend.reshape(seq_len, head_cols), out_all, (((1,), (1,)), ((), ())),
        preferred_element_type=jnp.float32,
    ).astype(jnp.bfloat16)
    target = gather_target(clean, noise, aux, partial)
    target_wide = target.astype(jnp.float32)
    spread = jnp.sqrt(jnp.sum(target_wide * target_wide) / (seq_len * model_width))
    scale = -loss_scale / (spread + target_floor)
    out_partial = (row_contract(target, attn_rows) * scale).astype(jnp.bfloat16)
    attn_grad = jnp.dot(target, out_all, preferred_element_type=jnp.float32) * scale
    attn_grad = attn_grad.astype(jnp.bfloat16).reshape(1, seq_len, heads_here, HEAD_DIM)
    qkv_grad = attend_back(attn_grad, attn_probs, probs_low, projected, score_scale)
    in_partial = row_contract(mixed_rows, qkv_grad.reshape(seq_len, 3 * head_cols))
    return scatter_all(dp_size, in_partial.astype(jnp.bfloat16), out_partial)


def solution(mesh):
    in_specs = (
        P("dp", "tensor", None),
        P("dp", "tensor", None),
        P("dp"),
        P("dp"),
        P(),
        P("dp", "tensor"),
        P("dp", "tensor"),
    )
    out_specs = (P("dp", "tensor"), P("dp", "tensor"))
    step = functools.partial(local, mesh.shape["dp"])
    return jax.shard_map(step, mesh=mesh, in_specs=in_specs, out_specs=out_specs, check_vma=False)
```

```python
import functools
import math

import jax
import jax.numpy as jnp
from jax import lax
from jax.experimental import pallas as pl
from jax.experimental.pallas import tpu as pltpu
from jax.sharding import PartitionSpec as P

HEAD_DIM = 128
STEPS = 1000


norm_eps = 1e-06
target_floor = 0.1


def time_terms(step_index, model_width):
    step_times = 1.4 * (step_index.astype(jnp.float32) + 0.5) / STEPS
    feature_ids = jnp.arange(model_width, dtype=jnp.float32)
    frequency = jnp.exp(-math.log(100.0) * feature_ids / model_width)
    phases = step_times[:, None] * frequency[None, :] + feature_ids[None, :]
    return (step_times, 0.5 * jnp.sin(phases), 0.5 * frequency[None, :] * jnp.cos(phases))


def low_einsum(form, left_part, right_part):
    return jnp.einsum(form, left_part, right_part, preferred_element_type=jnp.float32)


def attend(projected, projected_rate, score_scale):
    query_part = projected[:, :, :, 0, :]
    key_part = projected[:, :, :, 1, :]
    value_part = projected[:, :, :, 2, :]
    query_rate = projected_rate[:, :, :, 0, :]
    key_rate = projected_rate[:, :, :, 1, :]
    value_rate = projected_rate[:, :, :, 2, :]
    scores = low_einsum("lqhd,lkhd->lhqk", query_part, key_part) * score_scale
    score_rate = (
        low_einsum("lqhd,lkhd->lhqk", query_rate, key_part)
        + low_einsum("lqhd,lkhd->lhqk", query_part, key_rate)
    ) * score_scale
    attn_probs = jax.nn.softmax(scores, axis=-1)
    probs_low = attn_probs.astype(jnp.bfloat16)
    prob_rate = attn_probs * (score_rate - jnp.sum(attn_probs * score_rate, axis=-1, keepdims=True))
    prob_rate_low = prob_rate.astype(jnp.bfloat16)
    attn_out = low_einsum("lhqk,lkhd->lqhd", probs_low, value_part)
    attn_rate = low_einsum("lhqk,lkhd->lqhd", prob_rate_low, value_part) + low_einsum(
        "lhqk,lkhd->lqhd", probs_low, value_rate
    )
    return (attn_probs, probs_low, attn_out, attn_rate)


def attend_back(attn_grad, attn_probs, probs_low, projected, score_scale):
    query_part = projected[:, :, :, 0, :]
    key_part = projected[:, :, :, 1, :]
    value_part = projected[:, :, :, 2, :]
    prob_grad = low_einsum("lqhd,lkhd->lhqk", attn_grad, value_part)
    value_grad = low_einsum("lhqk,lqhd->lkhd", probs_low, attn_grad)
    score_grad = (
        attn_probs
        * (prob_grad - jnp.sum(attn_probs * prob_grad, axis=-1, keepdims=True))
        * score_scale
    ).astype(jnp.bfloat16)
    query_grad = low_einsum("lhqk,lkhd->lqhd", score_grad, key_part)
    key_grad = low_einsum("lhqk,lqhd->lkhd", score_grad, query_part)
    return jnp.stack([query_grad, key_grad, value_grad], axis=3).astype(jnp.bfloat16)


def row_contract(left_part, right_part):
    return lax.dot_general(
        left_part, right_part, (((0,), (0,)), ((), ())), preferred_element_type=jnp.float32
    )


MESH = pl.DeviceIdType.MESH
VMEM = pl.BlockSpec(memory_space=pltpu.VMEM)
HBM = pl.BlockSpec(memory_space=pl.ANY)


def places():
    dp_here, tensor_here = lax.axis_index("dp"), lax.axis_index("tensor")
    sibling = tensor_here + 1 - 2 * lax.rem(tensor_here, 2)
    opposite = lax.rem(tensor_here + 2, 4)
    diagonal = lax.rem(sibling + 2, 4)
    return dp_here, tensor_here, sibling, opposite, diagonal


def greet(devices):
    barrier = pltpu.get_barrier_semaphore()
    for device in devices:
        pl.semaphore_signal(barrier, inc=1, device_id=device, device_id_type=MESH)
    pl.semaphore_wait(barrier, len(devices))


def remote(source, target, send_sem, recv_sem, device):
    return pltpu.make_async_remote_copy(
        src_ref=source,
        dst_ref=target,
        send_sem=send_sem,
        recv_sem=recv_sem,
        device_id=device,
        device_id_type=MESH,
    )


def rows_of(ref, index, count):
    return ref.at[pl.ds(pl.multiple_of(index * count, count), count)]


def gather_kernel(
    dp_size, clean, noise, aux, w_qkv, w_out, mixed_all, rate_all, qkv_all, out_all,
    mixed, rate, w_send, w_recv, p_send, p_recv, t_send, t_recv, own_sem,
):
    dp_here, tensor_here, sibling, opposite, diagonal = places()
    part = clean.shape[0]
    qkv_rows = w_qkv.shape[0]
    outer = dp_size // 2
    outer_here, pair_here = dp_here // 2, lax.rem(dp_here, 2)
    onward = (lax.rem(outer_here + 1, outer) * 2 + pair_here, tensor_here)
    backward = (lax.rem(outer_here + outer - 1, outer) * 2 + pair_here, tensor_here)
    partner = (outer_here * 2 + 1 - pair_here, tensor_here)
    greet([onward, backward, partner, (dp_here, sibling), (dp_here, opposite)])
    pieces = min(2, qkv_rows // 16)
    piece = qkv_rows // pieces
    ring_copies, pair_copies = {}, []

    def ring_step(step):
        block = lax.rem(outer_here - step + outer, outer) * 2 + pair_here
        for which, (held, full) in enumerate(((w_qkv, qkv_all), (w_out, out_all))):
            for index in range(pieces):
                spot = rows_of(full, block * pieces + index, piece)
                source = held.at[pl.ds(index * piece, piece)] if step == 0 else spot
                if step > 0:
                    ring_copies[step - 1, which, index].wait_recv()
                if step < outer - 1:
                    copy = remote(
                        source, spot, w_send.at[step, which, index], w_recv.at[step, which, index], onward
                    )
                    copy.start()
                    ring_copies[step, which, index] = copy
                copy = remote(source, spot, p_send.at[step, which, index], p_recv.at[step, which, index], partner)
                copy.start()
                pair_copies.append(copy)

    ring_step(0)
    local_copies = [
        pltpu.make_async_copy(w_qkv, rows_of(qkv_all, dp_here, qkv_rows), own_sem.at[0]),
        pltpu.make_async_copy(w_out, rows_of(out_all, dp_here, qkv_rows), own_sem.at[1]),
    ]
    for copy in local_copies:
        copy.start()
    cos_t, sin_t = aux[3:4, :], aux[4:5, :]
    scale_up, amp_rate, offset = aux[0:1, :], aux[1:2, :], aux[2:3, :]

    @pl.loop(0, part // 16)
    def _(index):
        rows = pl.ds(pl.multiple_of(index * 16, 16), 16)
        clean_wide = clean[rows, :].astype(jnp.float32)
        noise_wide = noise[rows, :].astype(jnp.float32)
        noisy = cos_t * clean_wide + sin_t * noise_wide
        velocity = cos_t * noise_wide - sin_t * clean_wide
        inverse = lax.rsqrt(jnp.mean(noisy * noisy, axis=-1, keepdims=True) + norm_eps)
        cross = jnp.mean(noisy * velocity, axis=-1, keepdims=True)
        normed = noisy * inverse
        normed_rate = velocity * inverse - noisy * (inverse * inverse * inverse * cross)
        mixed[rows, :] = (normed * scale_up + offset).astype(jnp.bfloat16)
        rate[rows, :] = (normed_rate * scale_up + normed * amp_rate).astype(jnp.bfloat16)

    sends, forwards = [], []
    for which, (held, full) in enumerate(((mixed, mixed_all), (rate, rate_all))):
        spot = rows_of(full, tensor_here, part)
        to_opposite = remote(held, spot, t_send.at[which, 0], t_recv.at[which, 0], (dp_here, opposite))
        to_opposite.start()
        to_sibling = remote(held, spot, t_send.at[which, 1], t_recv.at[which, 1], (dp_here, sibling))
        to_sibling.start()
        own = pltpu.make_async_copy(held, spot, own_sem.at[2 + which])
        own.start()
        local_copies.append(own)
        arrived = rows_of(full, opposite, part)
        forward = remote(arrived, arrived, t_send.at[which, 2], t_recv.at[which, 2], (dp_here, sibling))
        sends.append((to_opposite, to_sibling))
        forwards.append(forward)
    for step in range(max(outer - 1, 2)):
        if step + 1 < outer:
            ring_step(step + 1)
        if step < 2:
            sends[step][0].wait_recv()
            forwards[step].start()
    for (to_opposite, to_sibling), forward in zip(sends, forwards):
        to_opposite.wait_send()
        to_sibling.wait()
        forward.wait()
    for copy in ring_copies.values():
        copy.wait_send()
    for copy in pair_copies:
        copy.wait()
    for copy in local_copies:
        copy.wait()


def gather_all(dp_size, clean, noise, aux, w_qkv, w_out):
    part, width = clean.shape
    low = jnp.bfloat16
    return pl.pallas_call(
        functools.partial(gather_kernel, dp_size),
        out_shape=(
            jax.ShapeDtypeStruct((4 * part, width), low),
            jax.ShapeDtypeStruct((4 * part, width), low),
            jax.ShapeDtypeStruct((dp_size * w_qkv.shape[0], w_qkv.shape[1]), low),
            jax.ShapeDtypeStruct((dp_size * w_out.shape[0], w_out.shape[1]), low),
        ),
        in_specs=[VMEM] * 5,
        out_specs=(HBM,) * 4,
        scratch_shapes=[
            pltpu.VMEM((part, width), low),
            pltpu.VMEM((part, width), low),
            pltpu.SemaphoreType.DMA((dp_size // 2, 2, 2)),
            pltpu.SemaphoreType.DMA((dp_size // 2, 2, 2)),
            pltpu.SemaphoreType.DMA((dp_size // 2, 2, 2)),
            pltpu.SemaphoreType.DMA((dp_size // 2, 2, 2)),
            pltpu.SemaphoreType.DMA((2, 3)),
            pltpu.SemaphoreType.DMA((2, 3)),
            pltpu.SemaphoreType.DMA((4,)),
        ],
        compiler_params=pltpu.CompilerParams(
            collective_id=0, has_side_effects=True, vmem_limit_bytes=32 * 2**20
        ),
    )(clean, noise, aux, w_qkv, w_out)


PIECES = 4


def target_kernel(
    clean, noise, aux, partial, target_all, first, from_sibling, from_opposite, summed, target,
    load_sem, r_send, r_recv, g_send, g_recv,
):
    dp_here, tensor_here, sibling, opposite, diagonal = places()
    part = clean.shape[0]
    piece = part // PIECES
    greet([(dp_here, sibling), (dp_here, opposite)])

    def block(owner, index):
        return rows_of(partial, owner * PIECES + index, piece)

    def slot(ref, index):
        return ref.at[pl.ds(index * piece, piece)]

    cross, direct, across, loads = [], [], [], []
    for index in range(PIECES):
        copy = remote(
            block(diagonal, index), slot(from_sibling.at[0], index), r_send.at[0, index], r_recv.at[0, index],
            (dp_here, sibling),
        )
        copy.start()
        cross.append(copy)
        load = pltpu.make_async_copy(block(opposite, index), slot(first.at[0], index), load_sem.at[0, index])
        load.start()
        loads.append(load)
    own_loads = []
    for index in range(PIECES):
        copy = remote(
            block(sibling, index), slot(from_sibling.at[1], index), r_send.at[1, index], r_recv.at[1, index],
            (dp_here, sibling),
        )
        copy.start()
        direct.append(copy)
        load = pltpu.make_async_copy(block(tensor_here, index), slot(first.at[1], index), load_sem.at[1, index])
        load.start()
        own_loads.append(load)
    for index in range(PIECES):
        cross[index].wait_recv()
        loads[index].wait()
        rows = pl.ds(index * piece, piece)
        total = first[0, rows, :].astype(jnp.float32) + from_sibling[0, rows, :].astype(jnp.float32)
        summed[rows, :] = total.astype(jnp.bfloat16)
        copy = remote(
            slot(summed, index), slot(from_opposite, index), r_send.at[2, index], r_recv.at[2, index],
            (dp_here, opposite),
        )
        copy.start()
        across.append(copy)
    cos_t, sin_t = aux[3:4, :], aux[4:5, :]
    sends, forwards = [], []

    def spot(owner, index):
        return rows_of(target_all, owner * PIECES + index, piece)

    for index in range(PIECES):
        across[index].wait_recv()
        direct[index].wait_recv()
        own_loads[index].wait()
        rows = pl.ds(index * piece, piece)
        clean_wide = clean[rows, :].astype(jnp.float32)
        noise_wide = noise[rows, :].astype(jnp.float32)
        noisy = cos_t * clean_wide + sin_t * noise_wide
        velocity = cos_t * noise_wide - sin_t * clean_wide
        moved = (
            first[1, rows, :].astype(jnp.float32)
            + from_sibling[1, rows, :].astype(jnp.float32)
            + from_opposite[rows, :].astype(jnp.float32)
        )
        value = -(cos_t * cos_t) * (noisy - velocity) - cos_t * sin_t * (noisy + velocity) - moved
        target[rows, :] = value.astype(jnp.bfloat16)
        held = slot(target, index)
        to_opposite = remote(
            held, spot(tensor_here, index), g_send.at[0, index], g_recv.at[0, index], (dp_here, opposite)
        )
        to_opposite.start()
        to_sibling = remote(
            held, spot(tensor_here, index), g_send.at[1, index], g_recv.at[1, index], (dp_here, sibling)
        )
        to_sibling.start()
        own = pltpu.make_async_copy(held, spot(tensor_here, index), load_sem.at[2, index])
        own.start()
        forward = remote(
            spot(opposite, index), spot(opposite, index), g_send.at[2, index], g_recv.at[2, index], (dp_here, sibling)
        )
        sends.append((to_opposite, to_sibling, own, forward))
    for to_opposite, to_sibling, own, forward in sends:
        to_opposite.wait_recv()
        forward.start()
    for index, (to_opposite, to_sibling, own, forward) in enumerate(sends):
        to_opposite.wait_send()
        to_sibling.wait()
        own.wait()
        forward.wait()
        cross[index].wait_send()
        direct[index].wait_send()
        across[index].wait_send()


def gather_target(clean, noise, aux, partial):
    part, width = clean.shape
    low = jnp.bfloat16
    return pl.pallas_call(
        target_kernel,
        out_shape=jax.ShapeDtypeStruct((4 * part, width), low),
        in_specs=[VMEM, VMEM, VMEM, HBM],
        out_specs=HBM,
        scratch_shapes=[
            pltpu.VMEM((2, part, width), low),
            pltpu.VMEM((2, part, width), low),
            pltpu.VMEM((part, width), low),
            pltpu.VMEM((part, width), low),
            pltpu.VMEM((part, width), low),
            pltpu.SemaphoreType.DMA((3, PIECES)),
            pltpu.SemaphoreType.DMA((3, PIECES)),
            pltpu.SemaphoreType.DMA((3, PIECES)),
            pltpu.SemaphoreType.DMA((3, PIECES)),
            pltpu.SemaphoreType.DMA((3, PIECES)),
        ],
        compiler_params=pltpu.CompilerParams(
            collective_id=1, has_side_effects=True, vmem_limit_bytes=32 * 2**20
        ),
    )(clean, noise, aux, partial)


def scatter_kernel(
    dp_size, in_partial, out_partial, in_sum, out_sum, in_own, out_own, in_pair, out_pair, in_ring, out_ring,
    in_sent, out_sent, p_send, p_recv, r_send, r_recv, own_sem,
):
    dp_here, tensor_here, _, _, _ = places()
    rows = in_sum.shape[0]
    outer = dp_size // 2
    outer_here, pair_here = dp_here // 2, lax.rem(dp_here, 2)
    onward = (lax.rem(outer_here + 1, outer) * 2 + pair_here, tensor_here)
    backward = (lax.rem(outer_here + outer - 1, outer) * 2 + pair_here, tensor_here)
    partner = (outer_here * 2 + 1 - pair_here, tensor_here)
    greet([onward, backward, partner])
    pieces = min(4, rows // 16)
    piece = rows // pieces
    arrays = (
        (out_partial, out_own, out_pair, out_ring, out_sent, out_sum),
        (in_partial, in_own, in_pair, in_ring, in_sent, in_sum),
    )
    loads, pair_copies, ring_copies = {}, {}, {}
    for step in range(outer):
        block = lax.rem(outer_here - step - 1 + outer, outer) * 2
        for which, (partial, own, pair, _, _, _) in enumerate(arrays):
            for index in range(pieces):
                copy = remote(
                    rows_of(partial, (block + 1 - pair_here) * pieces + index, piece),
                    pair.at[step, pl.ds(index * piece, piece)],
                    p_send.at[step, which, index], p_recv.at[step, which, index], partner,
                )
                copy.start()
                pair_copies[step, which, index] = copy
            load = pltpu.make_async_copy(
                rows_of(partial, block + pair_here, rows), own.at[step], own_sem.at[step, which]
            )
            load.start()
            loads[step, which] = load
    for step in range(outer):
        for which, (_, own, pair, ring, sent, total) in enumerate(arrays):
            loads[step, which].wait()
            for index in range(pieces):
                spot = pl.ds(index * piece, piece)
                pair_copies[step, which, index].wait_recv()
                value = own[step, spot, :].astype(jnp.float32) + pair[step, spot, :].astype(jnp.float32)
                if step > 0:
                    ring_copies[step - 1, which, index].wait_recv()
                    value = value + ring[step - 1, spot, :].astype(jnp.float32)
                if step == outer - 1:
                    total[spot, :] = value
                    continue
                sent[step, spot, :] = value.astype(jnp.bfloat16)
                copy = remote(
                    sent.at[step, spot], ring.at[step, spot],
                    r_send.at[step, which, index], r_recv.at[step, which, index], onward,
                )
                copy.start()
                ring_copies[step, which, index] = copy
    for copy in pair_copies.values():
        copy.wait_send()
    for copy in ring_copies.values():
        copy.wait_send()


def scatter_all(dp_size, in_partial, out_partial):
    rows = in_partial.shape[0] // dp_size
    in_cols, out_cols = in_partial.shape[1], out_partial.shape[1]
    low = jnp.bfloat16
    outer = dp_size // 2
    return pl.pallas_call(
        functools.partial(scatter_kernel, dp_size),
        out_shape=(
            jax.ShapeDtypeStruct((rows, in_cols), jnp.float32),
            jax.ShapeDtypeStruct((rows, out_cols), jnp.float32),
        ),
        in_specs=[HBM, HBM],
        out_specs=(VMEM, VMEM),
        scratch_shapes=[pltpu.VMEM((outer, rows, cols), low) for _ in range(4) for cols in (in_cols, out_cols)]
        + [pltpu.SemaphoreType.DMA((outer, 2, 4)) for _ in range(4)]
        + [pltpu.SemaphoreType.DMA((outer, 2))],
        compiler_params=pltpu.CompilerParams(
            collective_id=2, has_side_effects=True, vmem_limit_bytes=32 * 2**20
        ),
    )(in_partial, out_partial)


def local(dp_size, clean_latents, noise_latents, step_index, labels, class_shift, w_qkv, w_out_t):
    latent_count, part_len, model_width = clean_latents.shape
    head_cols = w_out_t.shape[1]
    heads_here = head_cols // HEAD_DIM
    score_scale = 1.0 / math.sqrt(HEAD_DIM)
    seq_len = part_len * 4
    loss_scale = 1.0 / math.sqrt(dp_size * latent_count * seq_len)
    step_times, amplitude, amp_rate = time_terms(step_index, model_width)
    offset = lax.dynamic_slice(class_shift, (labels[0], 0), (1, model_width)).astype(jnp.float32)
    cos_t, sin_t = jnp.cos(step_times[0]), jnp.sin(step_times[0])
    row = (1, model_width)
    aux = jnp.concatenate(
        [
            1.0 + amplitude,
            amp_rate,
            offset,
            jnp.broadcast_to(cos_t, row),
            jnp.broadcast_to(sin_t, row),
            jnp.zeros((3, model_width), jnp.float32),
        ]
    )
    clean, noise = clean_latents[0], noise_latents[0]
    mixed_rows, rate_rows, qkv_all, out_all = gather_all(dp_size, clean, noise, aux, w_qkv, w_out_t)
    heads_shape = (1, seq_len, heads_here, 3, HEAD_DIM)
    projected = jnp.dot(mixed_rows, qkv_all, preferred_element_type=jnp.float32)
    projected_rate = jnp.dot(rate_rows, qkv_all, preferred_element_type=jnp.float32)
    projected = projected.astype(jnp.bfloat16).reshape(heads_shape)
    projected_rate = projected_rate.astype(jnp.bfloat16).reshape(heads_shape)
    attn_probs, probs_low, attn_out, attn_rate = attend(projected, projected_rate, score_scale)
    attn_rows = attn_out.astype(jnp.bfloat16).reshape(seq_len, head_cols)
    blend = (cos_t * cos_t * attn_out + cos_t * sin_t * attn_rate).astype(jnp.bfloat16)
    partial = lax.dot_general(
        blend.reshape(seq_len, head_cols), out_all, (((1,), (1,)), ((), ())),
        preferred_element_type=jnp.float32,
    ).astype(jnp.bfloat16)
    target = gather_target(clean, noise, aux, partial)
    target_wide = target.astype(jnp.float32)
    spread = jnp.sqrt(jnp.sum(target_wide * target_wide) / (seq_len * model_width))
    scale = -loss_scale / (spread + target_floor)
    out_partial = (row_contract(target, attn_rows) * scale).astype(jnp.bfloat16)
    attn_grad = jnp.dot(target, out_all, preferred_element_type=jnp.float32) * scale
    attn_grad = attn_grad.astype(jnp.bfloat16).reshape(1, seq_len, heads_here, HEAD_DIM)
    qkv_grad = attend_back(attn_grad, attn_probs, probs_low, projected, score_scale)
    in_partial = row_contract(mixed_rows, qkv_grad.reshape(seq_len, 3 * head_cols))
    return scatter_all(dp_size, in_partial.astype(jnp.bfloat16), out_partial)


def solution(mesh):
    in_specs = (
        P("dp", "tensor", None),
        P("dp", "tensor", None),
        P("dp"),
        P("dp"),
        P(),
        P("dp", "tensor"),
        P("dp", "tensor"),
    )
    out_specs = (P("dp", "tensor"), P("dp", "tensor"))
    step = functools.partial(local, mesh.shape["dp"])
    return jax.shard_map(step, mesh=mesh, in_specs=in_specs, out_specs=out_specs, check_vma=False)
```

```python
import functools
import math

import jax
import jax.numpy as jnp
from jax import lax
from jax.experimental import pallas as pl
from jax.experimental.pallas import tpu as pltpu
from jax.sharding import PartitionSpec as P

HEAD_DIM = 128
STEPS = 1000


norm_eps = 1e-06
target_floor = 0.1


def time_terms(step_index, model_width):
    step_times = 1.4 * (step_index.astype(jnp.float32) + 0.5) / STEPS
    feature_ids = jnp.arange(model_width, dtype=jnp.float32)
    frequency = jnp.exp(-math.log(100.0) * feature_ids / model_width)
    phases = step_times[:, None] * frequency[None, :] + feature_ids[None, :]
    return (step_times, 0.5 * jnp.sin(phases), 0.5 * frequency[None, :] * jnp.cos(phases))


def low_einsum(form, left_part, right_part):
    return jnp.einsum(form, left_part, right_part, preferred_element_type=jnp.float32)


def attend(projected, projected_rate, score_scale):
    query_part = projected[:, :, :, 0, :]
    key_part = projected[:, :, :, 1, :]
    value_part = projected[:, :, :, 2, :]
    query_rate = projected_rate[:, :, :, 0, :]
    key_rate = projected_rate[:, :, :, 1, :]
    value_rate = projected_rate[:, :, :, 2, :]
    scores = low_einsum("lqhd,lkhd->lhqk", query_part, key_part) * score_scale
    score_rate = (
        low_einsum("lqhd,lkhd->lhqk", query_rate, key_part)
        + low_einsum("lqhd,lkhd->lhqk", query_part, key_rate)
    ) * score_scale
    attn_probs = jax.nn.softmax(scores, axis=-1)
    probs_low = attn_probs.astype(jnp.bfloat16)
    prob_rate = attn_probs * (score_rate - jnp.sum(attn_probs * score_rate, axis=-1, keepdims=True))
    prob_rate_low = prob_rate.astype(jnp.bfloat16)
    attn_out = low_einsum("lhqk,lkhd->lqhd", probs_low, value_part)
    attn_rate = low_einsum("lhqk,lkhd->lqhd", prob_rate_low, value_part) + low_einsum(
        "lhqk,lkhd->lqhd", probs_low, value_rate
    )
    return (attn_probs, probs_low, attn_out, attn_rate)


MESH = pl.DeviceIdType.MESH
VMEM = pl.BlockSpec(memory_space=pltpu.VMEM)
HBM = pl.BlockSpec(memory_space=pl.ANY)


def places():
    dp_here, tensor_here = lax.axis_index("dp"), lax.axis_index("tensor")
    sibling = tensor_here + 1 - 2 * lax.rem(tensor_here, 2)
    opposite = lax.rem(tensor_here + 2, 4)
    diagonal = lax.rem(sibling + 2, 4)
    return dp_here, tensor_here, sibling, opposite, diagonal


def greet(devices):
    barrier = pltpu.get_barrier_semaphore()
    for device in devices:
        pl.semaphore_signal(barrier, inc=1, device_id=device, device_id_type=MESH)
    pl.semaphore_wait(barrier, len(devices))


def remote(source, target, send_sem, recv_sem, device):
    return pltpu.make_async_remote_copy(
        src_ref=source,
        dst_ref=target,
        send_sem=send_sem,
        recv_sem=recv_sem,
        device_id=device,
        device_id_type=MESH,
    )


def rows_of(ref, index, count):
    return ref.at[pl.ds(pl.multiple_of(index * count, count), count)]


def gather_kernel(
    dp_size, clean, noise, aux, w_qkv, w_out, mixed_all, rate_all, qkv_all, out_all,
    clean_held, noise_held, mixed, rate, w_send, w_recv, p_send, p_recv, t_send, t_recv, own_sem,
):
    dp_here, tensor_here, sibling, opposite, diagonal = places()
    part = clean.shape[0]
    qkv_rows = w_qkv.shape[0]
    latent_loads = [
        pltpu.make_async_copy(clean, clean_held, own_sem.at[4]),
        pltpu.make_async_copy(noise, noise_held, own_sem.at[5]),
    ]
    for copy in latent_loads:
        copy.start()
    outer = dp_size // 2
    outer_here, pair_here = dp_here // 2, lax.rem(dp_here, 2)
    onward = (lax.rem(outer_here + 1, outer) * 2 + pair_here, tensor_here)
    backward = (lax.rem(outer_here + outer - 1, outer) * 2 + pair_here, tensor_here)
    partner = (outer_here * 2 + 1 - pair_here, tensor_here)
    greet([onward, backward, partner, (dp_here, sibling), (dp_here, opposite)])
    pieces = min(2, qkv_rows // 16)
    piece = qkv_rows // pieces
    ring_copies, pair_copies = {}, []

    def ring_step(step):
        block = lax.rem(outer_here - step + outer, outer) * 2 + pair_here
        for which, (held, full) in enumerate(((w_qkv, qkv_all), (w_out, out_all))):
            for index in range(pieces):
                spot = rows_of(full, block * pieces + index, piece)
                source = held.at[pl.ds(index * piece, piece)] if step == 0 else spot
                if step > 0:
                    ring_copies[step - 1, which, index].wait_recv()
                if step < outer - 1:
                    copy = remote(
                        source, spot, w_send.at[step, which, index], w_recv.at[step, which, index], onward
                    )
                    copy.start()
                    ring_copies[step, which, index] = copy
                copy = remote(source, spot, p_send.at[step, which, index], p_recv.at[step, which, index], partner)
                copy.start()
                pair_copies.append(copy)

    ring_step(0)
    local_copies = [
        pltpu.make_async_copy(w_qkv, rows_of(qkv_all, dp_here, qkv_rows), own_sem.at[0]),
        pltpu.make_async_copy(w_out, rows_of(out_all, dp_here, qkv_rows), own_sem.at[1]),
    ]
    for copy in local_copies:
        copy.start()
    for copy in latent_loads:
        copy.wait()
    cos_t, sin_t = aux[3:4, :], aux[4:5, :]
    scale_up, amp_rate, offset = aux[0:1, :], aux[1:2, :], aux[2:3, :]

    @pl.loop(0, part // 16)
    def _(index):
        rows = pl.ds(pl.multiple_of(index * 16, 16), 16)
        clean_wide = clean_held[rows, :].astype(jnp.float32)
        noise_wide = noise_held[rows, :].astype(jnp.float32)
        noisy = cos_t * clean_wide + sin_t * noise_wide
        velocity = cos_t * noise_wide - sin_t * clean_wide
        inverse = lax.rsqrt(jnp.mean(noisy * noisy, axis=-1, keepdims=True) + norm_eps)
        cross = jnp.mean(noisy * velocity, axis=-1, keepdims=True)
        normed = noisy * inverse
        normed_rate = velocity * inverse - noisy * (inverse * inverse * inverse * cross)
        mixed[rows, :] = (normed * scale_up + offset).astype(jnp.bfloat16)
        rate[rows, :] = (normed_rate * scale_up + normed * amp_rate).astype(jnp.bfloat16)

    sends, forwards = [], []
    for which, (held, full) in enumerate(((mixed, mixed_all), (rate, rate_all))):
        spot = rows_of(full, tensor_here, part)
        to_opposite = remote(held, spot, t_send.at[which, 0], t_recv.at[which, 0], (dp_here, opposite))
        to_opposite.start()
        to_sibling = remote(held, spot, t_send.at[which, 1], t_recv.at[which, 1], (dp_here, sibling))
        to_sibling.start()
        own = pltpu.make_async_copy(held, spot, own_sem.at[2 + which])
        own.start()
        local_copies.append(own)
        arrived = rows_of(full, opposite, part)
        forward = remote(arrived, arrived, t_send.at[which, 2], t_recv.at[which, 2], (dp_here, sibling))
        sends.append((to_opposite, to_sibling))
        forwards.append(forward)
    for step in range(max(outer - 1, 2)):
        if step + 1 < outer:
            ring_step(step + 1)
        if step < 2:
            sends[step][0].wait_recv()
            forwards[step].start()
    for (to_opposite, to_sibling), forward in zip(sends, forwards):
        to_opposite.wait_send()
        to_sibling.wait()
        forward.wait()
    for copy in ring_copies.values():
        copy.wait_send()
    for copy in pair_copies:
        copy.wait()
    for copy in local_copies:
        copy.wait()


def gather_all(dp_size, clean, noise, aux, w_qkv, w_out):
    part, width = clean.shape
    low = jnp.bfloat16
    return pl.pallas_call(
        functools.partial(gather_kernel, dp_size),
        out_shape=(
            jax.ShapeDtypeStruct((4 * part, width), low),
            jax.ShapeDtypeStruct((4 * part, width), low),
            jax.ShapeDtypeStruct((dp_size * w_qkv.shape[0], w_qkv.shape[1]), low),
            jax.ShapeDtypeStruct((dp_size * w_out.shape[0], w_out.shape[1]), low),
        ),
        in_specs=[HBM, HBM, VMEM, HBM, HBM],
        out_specs=(HBM,) * 4,
        scratch_shapes=[
            pltpu.VMEM((part, width), low),
            pltpu.VMEM((part, width), low),
            pltpu.VMEM((part, width), low),
            pltpu.VMEM((part, width), low),
            pltpu.SemaphoreType.DMA((dp_size // 2, 2, 2)),
            pltpu.SemaphoreType.DMA((dp_size // 2, 2, 2)),
            pltpu.SemaphoreType.DMA((dp_size // 2, 2, 2)),
            pltpu.SemaphoreType.DMA((dp_size // 2, 2, 2)),
            pltpu.SemaphoreType.DMA((2, 3)),
            pltpu.SemaphoreType.DMA((2, 3)),
            pltpu.SemaphoreType.DMA((6,)),
        ],
        compiler_params=pltpu.CompilerParams(
            collective_id=0, has_side_effects=True, vmem_limit_bytes=60 * 2**20
        ),
    )(clean, noise, aux, w_qkv, w_out)


PIECES = 4


def target_kernel(
    clean, noise, aux, partial, target_all, first, from_sibling, from_opposite, summed, target,
    load_sem, r_send, r_recv, g_send, g_recv,
):
    dp_here, tensor_here, sibling, opposite, diagonal = places()
    part = clean.shape[0]
    piece = part // PIECES
    greet([(dp_here, sibling), (dp_here, opposite)])

    def block(owner, index):
        return rows_of(partial, owner * PIECES + index, piece)

    def slot(ref, index):
        return ref.at[pl.ds(index * piece, piece)]

    cross, direct, across, loads = [], [], [], []
    for index in range(PIECES):
        copy = remote(
            block(diagonal, index), slot(from_sibling.at[0], index), r_send.at[0, index], r_recv.at[0, index],
            (dp_here, sibling),
        )
        copy.start()
        cross.append(copy)
        load = pltpu.make_async_copy(block(opposite, index), slot(first.at[0], index), load_sem.at[0, index])
        load.start()
        loads.append(load)
    own_loads = []
    for index in range(PIECES):
        copy = remote(
            block(sibling, index), slot(from_sibling.at[1], index), r_send.at[1, index], r_recv.at[1, index],
            (dp_here, sibling),
        )
        copy.start()
        direct.append(copy)
        load = pltpu.make_async_copy(block(tensor_here, index), slot(first.at[1], index), load_sem.at[1, index])
        load.start()
        own_loads.append(load)
    for index in range(PIECES):
        cross[index].wait_recv()
        loads[index].wait()
        rows = pl.ds(index * piece, piece)
        total = first[0, rows, :].astype(jnp.float32) + from_sibling[0, rows, :].astype(jnp.float32)
        summed[rows, :] = total.astype(jnp.bfloat16)
        copy = remote(
            slot(summed, index), slot(from_opposite, index), r_send.at[2, index], r_recv.at[2, index],
            (dp_here, opposite),
        )
        copy.start()
        across.append(copy)
    cos_t, sin_t = aux[3:4, :], aux[4:5, :]
    sends, forwards = [], []

    def spot(owner, index):
        return rows_of(target_all, owner * PIECES + index, piece)

    for index in range(PIECES):
        across[index].wait_recv()
        direct[index].wait_recv()
        own_loads[index].wait()
        rows = pl.ds(index * piece, piece)
        clean_wide = clean[rows, :].astype(jnp.float32)
        noise_wide = noise[rows, :].astype(jnp.float32)
        noisy = cos_t * clean_wide + sin_t * noise_wide
        velocity = cos_t * noise_wide - sin_t * clean_wide
        moved = (
            first[1, rows, :].astype(jnp.float32)
            + from_sibling[1, rows, :].astype(jnp.float32)
            + from_opposite[rows, :].astype(jnp.float32)
        )
        value = -(cos_t * cos_t) * (noisy - velocity) - cos_t * sin_t * (noisy + velocity) - moved
        target[rows, :] = value.astype(jnp.bfloat16)
        held = slot(target, index)
        to_opposite = remote(
            held, spot(tensor_here, index), g_send.at[0, index], g_recv.at[0, index], (dp_here, opposite)
        )
        to_opposite.start()
        to_sibling = remote(
            held, spot(tensor_here, index), g_send.at[1, index], g_recv.at[1, index], (dp_here, sibling)
        )
        to_sibling.start()
        own = pltpu.make_async_copy(held, spot(tensor_here, index), load_sem.at[2, index])
        own.start()
        forward = remote(
            spot(opposite, index), spot(opposite, index), g_send.at[2, index], g_recv.at[2, index], (dp_here, sibling)
        )
        sends.append((to_opposite, to_sibling, own, forward))
    for to_opposite, to_sibling, own, forward in sends:
        to_opposite.wait_recv()
        forward.start()
    for index, (to_opposite, to_sibling, own, forward) in enumerate(sends):
        to_opposite.wait_send()
        to_sibling.wait()
        own.wait()
        forward.wait()
        cross[index].wait_send()
        direct[index].wait_send()
        across[index].wait_send()


def gather_target(clean, noise, aux, partial):
    part, width = clean.shape
    low = jnp.bfloat16
    return pl.pallas_call(
        target_kernel,
        out_shape=jax.ShapeDtypeStruct((4 * part, width), low),
        in_specs=[VMEM, VMEM, VMEM, HBM],
        out_specs=HBM,
        scratch_shapes=[
            pltpu.VMEM((2, part, width), low),
            pltpu.VMEM((2, part, width), low),
            pltpu.VMEM((part, width), low),
            pltpu.VMEM((part, width), low),
            pltpu.VMEM((part, width), low),
            pltpu.SemaphoreType.DMA((3, PIECES)),
            pltpu.SemaphoreType.DMA((3, PIECES)),
            pltpu.SemaphoreType.DMA((3, PIECES)),
            pltpu.SemaphoreType.DMA((3, PIECES)),
            pltpu.SemaphoreType.DMA((3, PIECES)),
        ],
        compiler_params=pltpu.CompilerParams(
            collective_id=1, has_side_effects=True, vmem_limit_bytes=32 * 2**20
        ),
    )(clean, noise, aux, partial)


def dot(left, right, left_dim, right_dim):
    return lax.dot_general(
        left, right, (((left_dim,), (right_dim,)), ((), ())), preferred_element_type=jnp.float32
    )


def back_kernel(
    dp_size, loss_scale, score_scale, target, attn_rows, out_all, mixed, projected, probs, in_sum, out_sum,
    in_full, out_full, in_low, out_low, in_pair, out_pair, in_ring, out_ring, in_sent, out_sent,
    attn_grad, qkv_grad, p_send, p_recv, r_send, r_recv,
):
    dp_here, tensor_here, _, _, _ = places()
    rows = in_sum.shape[0]
    seq_len, width = target.shape
    outer = dp_size // 2
    outer_here, pair_here = dp_here // 2, lax.rem(dp_here, 2)
    onward = (lax.rem(outer_here + 1, outer) * 2 + pair_here, tensor_here)
    backward = (lax.rem(outer_here + outer - 1, outer) * 2 + pair_here, tensor_here)
    partner = (outer_here * 2 + 1 - pair_here, tensor_here)
    greet([onward, backward, partner])
    pieces = min(4, rows // 16)
    piece = rows // pieces
    out_set = (out_full, out_low, out_pair, out_ring, out_sent, out_sum)
    in_set = (in_full, in_low, in_pair, in_ring, in_sent, in_sum)
    pair_copies, ring_copies = {}, {}

    def squares(index, held):
        spot = pl.ds(pl.multiple_of(index * 16, 16), 16)
        value = target[spot, :].astype(jnp.float32)
        return held + value * value

    total = lax.fori_loop(0, seq_len // 16, squares, jnp.zeros((16, width), jnp.float32))
    total = jnp.sum(jnp.sum(total, axis=0, keepdims=True), axis=1, keepdims=True)
    scale = -loss_scale / (jnp.sqrt(total / (seq_len * width)) + target_floor)

    def out_chunk(spot):
        return dot(target[:, spot], attn_rows[...], 0, 0) * scale

    def in_chunk(spot):
        return dot(mixed[:, spot], qkv_grad[...], 0, 0)

    def block_of(step):
        return lax.rem(outer_here - step - 1 + outer, outer) * 2

    def send_pair(step, which, low, pair):
        for index in range(pieces):
            copy = remote(
                rows_of(low, (block_of(step) + 1 - pair_here) * pieces + index, piece),
                pair.at[step, pl.ds(index * piece, piece)],
                p_send.at[step, which, index], p_recv.at[step, which, index], partner,
            )
            copy.start()
            pair_copies[step, which, index] = copy

    def make_all(which, chunk, arrays):
        full, low, pair = arrays[:3]
        if rows % 128 == 0:
            for step in range(outer):
                spot = pl.ds(pl.multiple_of((block_of(step) + 1 - pair_here) * rows, rows), rows)
                low[spot, :] = chunk(spot).astype(jnp.bfloat16)
                send_pair(step, which, low, pair)
            for step in range(outer):
                spot = pl.ds(pl.multiple_of((block_of(step) + pair_here) * rows, rows), rows)
                full[spot, :] = chunk(spot)
        else:

            @pl.loop(0, width // 128)
            def _(index):
                spot = pl.ds(pl.multiple_of(index * 128, 128), 128)
                value = chunk(spot)
                full[spot, :] = value
                low[spot, :] = value.astype(jnp.bfloat16)

            for step in range(outer):
                send_pair(step, which, low, pair)

    def ring_step(step, which, arrays):
        full, _, pair, ring, sent, total = arrays
        for index in range(pieces):
            spot = pl.ds(index * piece, piece)
            own = pl.ds(pl.multiple_of((block_of(step) + pair_here) * rows + index * piece, piece), piece)
            pair_copies[step, which, index].wait_recv()
            value = full[own, :] + pair[step, spot, :].astype(jnp.float32)
            if step > 0:
                ring_copies[step - 1, which, index].wait_recv()
                value = value + ring[step - 1, spot, :].astype(jnp.float32)
            if step == outer - 1:
                total[spot, :] = value
                continue
            sent[step, spot, :] = value.astype(jnp.bfloat16)
            copy = remote(
                sent.at[step, spot], ring.at[step, spot],
                r_send.at[step, which, index], r_recv.at[step, which, index], onward,
            )
            copy.start()
            ring_copies[step, which, index] = copy

    make_all(0, out_chunk, out_set)
    tile = min(256, seq_len)
    for start in range(0, seq_len, tile):
        spot = pl.ds(start, tile)
        attn_grad[spot, :] = (dot(target[spot, :], out_all[...], 1, 0) * scale).astype(jnp.bfloat16)
    ring_step(0, 0, out_set)
    done = 1
    for head in range(probs.shape[0]):
        base = head * 3 * HEAD_DIM
        query = projected[:, base : base + HEAD_DIM]
        key = projected[:, base + HEAD_DIM : base + 2 * HEAD_DIM]
        value = projected[:, base + 2 * HEAD_DIM : base + 3 * HEAD_DIM]
        key_grad = jnp.zeros((seq_len, HEAD_DIM), jnp.float32)
        value_grad = jnp.zeros((seq_len, HEAD_DIM), jnp.float32)
        for start in range(0, seq_len, tile):
            spot = pl.ds(start, tile)
            grad = attn_grad[spot, head * HEAD_DIM : (head + 1) * HEAD_DIM]
            prob = probs[head, spot, :]
            prob_grad = dot(grad, value, 1, 1)
            inner = jnp.sum(prob * prob_grad, axis=-1, keepdims=True)
            score_grad = (prob * (prob_grad - inner) * score_scale).astype(jnp.bfloat16)
            qkv_grad[spot, base : base + HEAD_DIM] = dot(score_grad, key, 1, 0).astype(jnp.bfloat16)
            key_grad = key_grad + dot(score_grad, query[start : start + tile], 0, 0)
            value_grad = value_grad + dot(prob.astype(jnp.bfloat16), grad, 0, 0)
        qkv_grad[:, base + HEAD_DIM : base + 2 * HEAD_DIM] = key_grad.astype(jnp.bfloat16)
        qkv_grad[:, base + 2 * HEAD_DIM : base + 3 * HEAD_DIM] = value_grad.astype(jnp.bfloat16)
        if done < outer - 1:
            ring_step(done, 0, out_set)
            done += 1
    make_all(1, in_chunk, in_set)
    for step in range(done, outer):
        ring_step(step, 0, out_set)
    for step in range(outer):
        ring_step(step, 1, in_set)
    for copy in pair_copies.values():
        copy.wait_send()
    for copy in ring_copies.values():
        copy.wait_send()


def back_all(dp_size, loss_scale, score_scale, target, attn_rows, out_all, mixed, projected, probs):
    width, out_cols = out_all.shape
    rows = width // dp_size
    in_cols = projected.shape[1]
    seq_len = target.shape[0]
    low = jnp.bfloat16
    outer = dp_size // 2
    both = (in_cols, out_cols)
    return pl.pallas_call(
        functools.partial(back_kernel, dp_size, loss_scale, score_scale),
        out_shape=(
            jax.ShapeDtypeStruct((rows, in_cols), jnp.float32),
            jax.ShapeDtypeStruct((rows, out_cols), jnp.float32),
        ),
        in_specs=[VMEM] * 6,
        out_specs=(VMEM, VMEM),
        scratch_shapes=[pltpu.VMEM((width, cols), jnp.float32) for cols in both]
        + [pltpu.VMEM((width, cols), low) for cols in both]
        + [pltpu.VMEM((outer, rows, cols), low) for _ in range(3) for cols in both]
        + [pltpu.VMEM((seq_len, out_cols), low), pltpu.VMEM((seq_len, in_cols), low)]
        + [pltpu.SemaphoreType.DMA((outer, 2, 4)) for _ in range(4)],
        compiler_params=pltpu.CompilerParams(
            collective_id=2, has_side_effects=True, vmem_limit_bytes=60 * 2**20
        ),
    )(target, attn_rows, out_all, mixed, projected, probs)


def local(dp_size, clean_latents, noise_latents, step_index, labels, class_shift, w_qkv, w_out_t):
    latent_count, part_len, model_width = clean_latents.shape
    head_cols = w_out_t.shape[1]
    heads_here = head_cols // HEAD_DIM
    score_scale = 1.0 / math.sqrt(HEAD_DIM)
    seq_len = part_len * 4
    loss_scale = 1.0 / math.sqrt(dp_size * latent_count * seq_len)
    step_times, amplitude, amp_rate = time_terms(step_index, model_width)
    offset = lax.dynamic_slice(class_shift, (labels[0], 0), (1, model_width)).astype(jnp.float32)
    cos_t, sin_t = jnp.cos(step_times[0]), jnp.sin(step_times[0])
    row = (1, model_width)
    aux = jnp.concatenate(
        [
            1.0 + amplitude,
            amp_rate,
            offset,
            jnp.broadcast_to(cos_t, row),
            jnp.broadcast_to(sin_t, row),
            jnp.zeros((3, model_width), jnp.float32),
        ]
    )
    clean, noise = clean_latents[0], noise_latents[0]
    mixed_rows, rate_rows, qkv_all, out_all = gather_all(dp_size, clean, noise, aux, w_qkv, w_out_t)
    heads_shape = (1, seq_len, heads_here, 3, HEAD_DIM)
    projected = jnp.dot(mixed_rows, qkv_all, preferred_element_type=jnp.float32)
    projected_rate = jnp.dot(rate_rows, qkv_all, preferred_element_type=jnp.float32)
    projected = projected.astype(jnp.bfloat16).reshape(heads_shape)
    projected_rate = projected_rate.astype(jnp.bfloat16).reshape(heads_shape)
    attn_probs, probs_low, attn_out, attn_rate = attend(projected, projected_rate, score_scale)
    attn_rows = attn_out.astype(jnp.bfloat16).reshape(seq_len, head_cols)
    blend = (cos_t * cos_t * attn_out + cos_t * sin_t * attn_rate).astype(jnp.bfloat16)
    partial = lax.dot_general(
        blend.reshape(seq_len, head_cols), out_all, (((1,), (1,)), ((), ())),
        preferred_element_type=jnp.float32,
    ).astype(jnp.bfloat16)
    target = gather_target(clean, noise, aux, partial)
    return back_all(
        dp_size, loss_scale, score_scale, target, attn_rows, out_all, mixed_rows,
        projected.reshape(seq_len, 3 * head_cols), attn_probs[0],
    )


def solution(mesh):
    in_specs = (
        P("dp", "tensor", None),
        P("dp", "tensor", None),
        P("dp"),
        P("dp"),
        P(),
        P("dp", "tensor"),
        P("dp", "tensor"),
    )
    out_specs = (P("dp", "tensor"), P("dp", "tensor"))
    step = functools.partial(local, mesh.shape["dp"])
    return jax.shard_map(step, mesh=mesh, in_specs=in_specs, out_specs=out_specs, check_vma=False)
```

```python
import functools
import math

import jax
import jax.numpy as jnp
from jax import lax
from jax.experimental import pallas as pl
from jax.experimental.pallas import tpu as pltpu
from jax.sharding import PartitionSpec as P

HEAD_DIM = 128
STEPS = 1000


norm_eps = 1e-06
target_floor = 0.1


def time_terms(step_index, model_width):
    step_times = 1.4 * (step_index.astype(jnp.float32) + 0.5) / STEPS
    feature_ids = jnp.arange(model_width, dtype=jnp.float32)
    frequency = jnp.exp(-math.log(100.0) * feature_ids / model_width)
    phases = step_times[:, None] * frequency[None, :] + feature_ids[None, :]
    return (step_times, 0.5 * jnp.sin(phases), 0.5 * frequency[None, :] * jnp.cos(phases))


MESH = pl.DeviceIdType.MESH
VMEM = pl.BlockSpec(memory_space=pltpu.VMEM)
HBM = pl.BlockSpec(memory_space=pl.ANY)


def places():
    dp_here, tensor_here = lax.axis_index("dp"), lax.axis_index("tensor")
    sibling = tensor_here + 1 - 2 * lax.rem(tensor_here, 2)
    opposite = lax.rem(tensor_here + 2, 4)
    diagonal = lax.rem(sibling + 2, 4)
    return dp_here, tensor_here, sibling, opposite, diagonal


def greet(devices):
    barrier = pltpu.get_barrier_semaphore()
    for device in devices:
        pl.semaphore_signal(barrier, inc=1, device_id=device, device_id_type=MESH)
    pl.semaphore_wait(barrier, len(devices))


def remote(source, target, send_sem, recv_sem, device):
    return pltpu.make_async_remote_copy(
        src_ref=source,
        dst_ref=target,
        send_sem=send_sem,
        recv_sem=recv_sem,
        device_id=device,
        device_id_type=MESH,
    )


def rows_of(ref, index, count):
    return ref.at[pl.ds(pl.multiple_of(index * count, count), count)]


def dot(left, right, left_dim, right_dim):
    return lax.dot_general(
        left, right, (((left_dim,), (right_dim,)), ((), ())), preferred_element_type=jnp.float32
    )


def gather_kernel(
    dp_size, score_scale, clean, noise, aux, w_qkv, w_out, mixed_all, rate_all, qkv_all, out_all,
    projected, probs, attn_rows, blend, mixed_held, rate_held, qkv_held, projected_rate,
    clean_held, noise_held, mixed, rate, w_send, w_recv, p_send, p_recv, t_send, t_recv, own_sem,
):
    dp_here, tensor_here, sibling, opposite, diagonal = places()
    part = clean.shape[0]
    qkv_rows = w_qkv.shape[0]
    latent_loads = [
        pltpu.make_async_copy(clean, clean_held, own_sem.at[4]),
        pltpu.make_async_copy(noise, noise_held, own_sem.at[5]),
    ]
    for copy in latent_loads:
        copy.start()
    outer = dp_size // 2
    outer_here, pair_here = dp_here // 2, lax.rem(dp_here, 2)
    onward = (lax.rem(outer_here + 1, outer) * 2 + pair_here, tensor_here)
    backward = (lax.rem(outer_here + outer - 1, outer) * 2 + pair_here, tensor_here)
    partner = (outer_here * 2 + 1 - pair_here, tensor_here)
    greet([onward, backward, partner, (dp_here, sibling), (dp_here, opposite)])
    pieces = min(2, qkv_rows // 16)
    piece = qkv_rows // pieces
    ring_copies, pair_copies = {}, {}

    def ring_step(step, which):
        block = lax.rem(outer_here - step + outer, outer) * 2 + pair_here
        held, full = ((w_qkv, qkv_all), (w_out, out_all))[which]
        for index in range(pieces):
            spot = rows_of(full, block * pieces + index, piece)
            source = held.at[pl.ds(index * piece, piece)] if step == 0 else spot
            if step > 0:
                ring_copies[step - 1, which, index].wait_recv()
            if step < outer - 1:
                copy = remote(
                    source, spot, w_send.at[step, which, index], w_recv.at[step, which, index], onward
                )
                copy.start()
                ring_copies[step, which, index] = copy
            copy = remote(source, spot, p_send.at[step, which, index], p_recv.at[step, which, index], partner)
            copy.start()
            pair_copies[step, which, index] = copy

    ring_step(0, 0)
    local_copies = [
        pltpu.make_async_copy(w_qkv, rows_of(qkv_all, dp_here, qkv_rows), own_sem.at[0]),
        pltpu.make_async_copy(w_out, rows_of(out_all, dp_here, qkv_rows), own_sem.at[1]),
    ]
    for copy in local_copies:
        copy.start()
    for copy in latent_loads:
        copy.wait()
    cos_t, sin_t = aux[3:4, :], aux[4:5, :]
    scale_up, amp_rate, offset = aux[0:1, :], aux[1:2, :], aux[2:3, :]

    @pl.loop(0, part // 16)
    def _(index):
        rows = pl.ds(pl.multiple_of(index * 16, 16), 16)
        clean_wide = clean_held[rows, :].astype(jnp.float32)
        noise_wide = noise_held[rows, :].astype(jnp.float32)
        noisy = cos_t * clean_wide + sin_t * noise_wide
        velocity = cos_t * noise_wide - sin_t * clean_wide
        inverse = lax.rsqrt(jnp.mean(noisy * noisy, axis=-1, keepdims=True) + norm_eps)
        cross = jnp.mean(noisy * velocity, axis=-1, keepdims=True)
        normed = noisy * inverse
        normed_rate = velocity * inverse - noisy * (inverse * inverse * inverse * cross)
        mixed[rows, :] = (normed * scale_up + offset).astype(jnp.bfloat16)
        rate[rows, :] = (normed_rate * scale_up + normed * amp_rate).astype(jnp.bfloat16)

    sends, forwards = [], []
    for which, (held, full) in enumerate(((mixed, mixed_all), (rate, rate_all))):
        spot = rows_of(full, tensor_here, part)
        to_opposite = remote(held, spot, t_send.at[which, 0], t_recv.at[which, 0], (dp_here, opposite))
        to_opposite.start()
        to_sibling = remote(held, spot, t_send.at[which, 1], t_recv.at[which, 1], (dp_here, sibling))
        to_sibling.start()
        own = pltpu.make_async_copy(held, spot, own_sem.at[2 + which])
        own.start()
        local_copies.append(own)
        arrived = rows_of(full, opposite, part)
        forward = remote(arrived, arrived, t_send.at[which, 2], t_recv.at[which, 2], (dp_here, sibling))
        sends.append((to_opposite, to_sibling))
        forwards.append(forward)
    for step in range(max(outer - 1, 2)):
        if step + 1 < outer:
            ring_step(step + 1, 0)
        if step < 2:
            sends[step][0].wait_recv()
            forwards[step].start()
    ring_step(0, 1)
    for copy in local_copies:
        copy.wait()
    loads = []
    for which, (full, held) in enumerate(((mixed_all, mixed_held), (rate_all, rate_held))):
        sends[which][1].wait_recv()
        forwards[which].wait_recv()
        load = pltpu.make_async_copy(full, held, own_sem.at[6 + which])
        load.start()
        loads.append(load)
    for (_, which, _), copy in pair_copies.items():
        if which == 0:
            copy.wait_recv()
    load = pltpu.make_async_copy(qkv_all, qkv_held, own_sem.at[8])
    load.start()
    loads.append(load)
    for load in loads:
        load.wait()
    seq_len = mixed_held.shape[0]
    tile = min(256, seq_len)
    for step, (held, result) in enumerate(((mixed_held, projected), (rate_held, projected_rate))):
        for start in range(0, seq_len, tile):
            spot = pl.ds(start, tile)
            result[spot, :] = dot(held[spot, :], qkv_held[...], 1, 0).astype(jnp.bfloat16)
        if step + 1 < outer:
            ring_step(step + 1, 1)
    cos_part, sin_part = aux[3:4, :HEAD_DIM], aux[4:5, :HEAD_DIM]
    done = 3
    for head in range(probs.shape[0]):
        base = head * 3 * HEAD_DIM
        columns = [slice(base + part * HEAD_DIM, base + (part + 1) * HEAD_DIM) for part in range(3)]
        key, key_rate = projected[:, columns[1]], projected_rate[:, columns[1]]
        value, value_rate = projected[:, columns[2]], projected_rate[:, columns[2]]
        here = slice(head * HEAD_DIM, (head + 1) * HEAD_DIM)
        for start in range(0, seq_len, tile):
            spot = pl.ds(start, tile)
            query, query_rate = projected[spot, columns[0]], projected_rate[spot, columns[0]]
            scores = dot(query, key, 1, 1) * score_scale
            score_rate = (dot(query_rate, key, 1, 1) + dot(query, key_rate, 1, 1)) * score_scale
            prob = jnp.exp(scores - jnp.max(scores, axis=-1, keepdims=True))
            prob = prob * (1.0 / jnp.sum(prob, axis=-1, keepdims=True))
            inner = jnp.sum(prob * score_rate, axis=-1, keepdims=True)
            prob_rate = (prob * (score_rate - inner)).astype(jnp.bfloat16)
            probs[head, spot, :] = prob
            prob_low = prob.astype(jnp.bfloat16)
            attn = dot(prob_low, value, 1, 0)
            attn_rate = dot(prob_rate, value, 1, 0) + dot(prob_low, value_rate, 1, 0)
            attn_rows[spot, here] = attn.astype(jnp.bfloat16)
            mix = cos_part * cos_part * attn + cos_part * sin_part * attn_rate
            blend[spot, here] = mix.astype(jnp.bfloat16)
        if done < outer:
            ring_step(done, 1)
            done += 1
    for step in range(done, outer):
        ring_step(step, 1)
    for (to_opposite, to_sibling), forward in zip(sends, forwards):
        to_opposite.wait_send()
        to_sibling.wait_send()
        forward.wait_send()
    for copy in ring_copies.values():
        copy.wait_send()
    for (_, which, _), copy in pair_copies.items():
        copy.wait_send()
        if which == 1:
            copy.wait_recv()


def gather_all(dp_size, score_scale, clean, noise, aux, w_qkv, w_out):
    part, width = clean.shape
    low = jnp.bfloat16
    seq_len, cols, head_cols = 4 * part, w_qkv.shape[1], w_out.shape[1]
    return pl.pallas_call(
        functools.partial(gather_kernel, dp_size, score_scale),
        out_shape=(
            jax.ShapeDtypeStruct((4 * part, width), low),
            jax.ShapeDtypeStruct((4 * part, width), low),
            jax.ShapeDtypeStruct((dp_size * w_qkv.shape[0], w_qkv.shape[1]), low),
            jax.ShapeDtypeStruct((dp_size * w_out.shape[0], w_out.shape[1]), low),
            jax.ShapeDtypeStruct((seq_len, cols), low),
            jax.ShapeDtypeStruct((head_cols // HEAD_DIM, seq_len, seq_len), jnp.float32),
            jax.ShapeDtypeStruct((seq_len, head_cols), low),
            jax.ShapeDtypeStruct((seq_len, head_cols), low),
        ),
        in_specs=[HBM, HBM, VMEM, HBM, HBM],
        out_specs=(HBM,) * 4 + (VMEM,) * 4,
        scratch_shapes=[
            pltpu.VMEM((seq_len, width), low),
            pltpu.VMEM((seq_len, width), low),
            pltpu.VMEM((dp_size * w_qkv.shape[0], cols), low),
            pltpu.VMEM((seq_len, cols), low),
            pltpu.VMEM((part, width), low),
            pltpu.VMEM((part, width), low),
            pltpu.VMEM((part, width), low),
            pltpu.VMEM((part, width), low),
            pltpu.SemaphoreType.DMA((dp_size // 2, 2, 2)),
            pltpu.SemaphoreType.DMA((dp_size // 2, 2, 2)),
            pltpu.SemaphoreType.DMA((dp_size // 2, 2, 2)),
            pltpu.SemaphoreType.DMA((dp_size // 2, 2, 2)),
            pltpu.SemaphoreType.DMA((2, 3)),
            pltpu.SemaphoreType.DMA((2, 3)),
            pltpu.SemaphoreType.DMA((9,)),
        ],
        compiler_params=pltpu.CompilerParams(
            collective_id=0, has_side_effects=True, vmem_limit_bytes=60 * 2**20
        ),
    )(clean, noise, aux, w_qkv, w_out)


PIECES = 4


def target_kernel(
    clean, noise, aux, partial, target_all, first, from_sibling, from_opposite, summed, target,
    load_sem, r_send, r_recv, g_send, g_recv,
):
    dp_here, tensor_here, sibling, opposite, diagonal = places()
    part = clean.shape[0]
    piece = part // PIECES
    greet([(dp_here, sibling), (dp_here, opposite)])

    def block(owner, index):
        return rows_of(partial, owner * PIECES + index, piece)

    def slot(ref, index):
        return ref.at[pl.ds(index * piece, piece)]

    cross, direct, across, loads = [], [], [], []
    for index in range(PIECES):
        copy = remote(
            block(diagonal, index), slot(from_sibling.at[0], index), r_send.at[0, index], r_recv.at[0, index],
            (dp_here, sibling),
        )
        copy.start()
        cross.append(copy)
        load = pltpu.make_async_copy(block(opposite, index), slot(first.at[0], index), load_sem.at[0, index])
        load.start()
        loads.append(load)
    own_loads = []
    for index in range(PIECES):
        copy = remote(
            block(sibling, index), slot(from_sibling.at[1], index), r_send.at[1, index], r_recv.at[1, index],
            (dp_here, sibling),
        )
        copy.start()
        direct.append(copy)
        load = pltpu.make_async_copy(block(tensor_here, index), slot(first.at[1], index), load_sem.at[1, index])
        load.start()
        own_loads.append(load)
    for index in range(PIECES):
        cross[index].wait_recv()
        loads[index].wait()
        rows = pl.ds(index * piece, piece)
        total = first[0, rows, :].astype(jnp.float32) + from_sibling[0, rows, :].astype(jnp.float32)
        summed[rows, :] = total.astype(jnp.bfloat16)
        copy = remote(
            slot(summed, index), slot(from_opposite, index), r_send.at[2, index], r_recv.at[2, index],
            (dp_here, opposite),
        )
        copy.start()
        across.append(copy)
    cos_t, sin_t = aux[3:4, :], aux[4:5, :]
    sends, forwards = [], []

    def spot(owner, index):
        return rows_of(target_all, owner * PIECES + index, piece)

    for index in range(PIECES):
        across[index].wait_recv()
        direct[index].wait_recv()
        own_loads[index].wait()
        rows = pl.ds(index * piece, piece)
        clean_wide = clean[rows, :].astype(jnp.float32)
        noise_wide = noise[rows, :].astype(jnp.float32)
        noisy = cos_t * clean_wide + sin_t * noise_wide
        velocity = cos_t * noise_wide - sin_t * clean_wide
        moved = (
            first[1, rows, :].astype(jnp.float32)
            + from_sibling[1, rows, :].astype(jnp.float32)
            + from_opposite[rows, :].astype(jnp.float32)
        )
        value = -(cos_t * cos_t) * (noisy - velocity) - cos_t * sin_t * (noisy + velocity) - moved
        target[rows, :] = value.astype(jnp.bfloat16)
        held = slot(target, index)
        to_opposite = remote(
            held, spot(tensor_here, index), g_send.at[0, index], g_recv.at[0, index], (dp_here, opposite)
        )
        to_opposite.start()
        to_sibling = remote(
            held, spot(tensor_here, index), g_send.at[1, index], g_recv.at[1, index], (dp_here, sibling)
        )
        to_sibling.start()
        own = pltpu.make_async_copy(held, spot(tensor_here, index), load_sem.at[2, index])
        own.start()
        forward = remote(
            spot(opposite, index), spot(opposite, index), g_send.at[2, index], g_recv.at[2, index], (dp_here, sibling)
        )
        sends.append((to_opposite, to_sibling, own, forward))
    for to_opposite, to_sibling, own, forward in sends:
        to_opposite.wait_recv()
        forward.start()
    for index, (to_opposite, to_sibling, own, forward) in enumerate(sends):
        to_opposite.wait_send()
        to_sibling.wait()
        own.wait()
        forward.wait()
        cross[index].wait_send()
        direct[index].wait_send()
        across[index].wait_send()


def gather_target(clean, noise, aux, partial):
    part, width = clean.shape
    low = jnp.bfloat16
    return pl.pallas_call(
        target_kernel,
        out_shape=jax.ShapeDtypeStruct((4 * part, width), low),
        in_specs=[VMEM, VMEM, VMEM, HBM],
        out_specs=HBM,
        scratch_shapes=[
            pltpu.VMEM((2, part, width), low),
            pltpu.VMEM((2, part, width), low),
            pltpu.VMEM((part, width), low),
            pltpu.VMEM((part, width), low),
            pltpu.VMEM((part, width), low),
            pltpu.SemaphoreType.DMA((3, PIECES)),
            pltpu.SemaphoreType.DMA((3, PIECES)),
            pltpu.SemaphoreType.DMA((3, PIECES)),
            pltpu.SemaphoreType.DMA((3, PIECES)),
            pltpu.SemaphoreType.DMA((3, PIECES)),
        ],
        compiler_params=pltpu.CompilerParams(
            collective_id=1, has_side_effects=True, vmem_limit_bytes=32 * 2**20
        ),
    )(clean, noise, aux, partial)


def back_kernel(
    dp_size, loss_scale, score_scale, target, attn_rows, out_all, mixed, projected, probs, in_sum, out_sum,
    in_full, out_full, in_low, out_low, in_pair, out_pair, in_ring, out_ring, in_sent, out_sent,
    attn_grad, qkv_grad, p_send, p_recv, r_send, r_recv,
):
    dp_here, tensor_here, _, _, _ = places()
    rows = in_sum.shape[0]
    seq_len, width = target.shape
    outer = dp_size // 2
    outer_here, pair_here = dp_here // 2, lax.rem(dp_here, 2)
    onward = (lax.rem(outer_here + 1, outer) * 2 + pair_here, tensor_here)
    backward = (lax.rem(outer_here + outer - 1, outer) * 2 + pair_here, tensor_here)
    partner = (outer_here * 2 + 1 - pair_here, tensor_here)
    greet([onward, backward, partner])
    pieces = min(4, rows // 16)
    piece = rows // pieces
    out_set = (out_full, out_low, out_pair, out_ring, out_sent, out_sum)
    in_set = (in_full, in_low, in_pair, in_ring, in_sent, in_sum)
    pair_copies, ring_copies = {}, {}

    def squares(index, held):
        spot = pl.ds(pl.multiple_of(index * 16, 16), 16)
        value = target[spot, :].astype(jnp.float32)
        return held + value * value

    total = lax.fori_loop(0, seq_len // 16, squares, jnp.zeros((16, width), jnp.float32))
    total = jnp.sum(jnp.sum(total, axis=0, keepdims=True), axis=1, keepdims=True)
    scale = -loss_scale / (jnp.sqrt(total / (seq_len * width)) + target_floor)

    def out_chunk(spot):
        return dot(target[:, spot], attn_rows[...], 0, 0) * scale

    def in_chunk(spot):
        return dot(mixed[:, spot], qkv_grad[...], 0, 0)

    def block_of(step):
        return lax.rem(outer_here - step - 1 + outer, outer) * 2

    def send_pair(step, which, low, pair):
        for index in range(pieces):
            copy = remote(
                rows_of(low, (block_of(step) + 1 - pair_here) * pieces + index, piece),
                pair.at[step, pl.ds(index * piece, piece)],
                p_send.at[step, which, index], p_recv.at[step, which, index], partner,
            )
            copy.start()
            pair_copies[step, which, index] = copy

    def make_all(which, chunk, arrays):
        full, low, pair = arrays[:3]
        if rows % 128 == 0:
            for step in range(outer):
                spot = pl.ds(pl.multiple_of((block_of(step) + 1 - pair_here) * rows, rows), rows)
                low[spot, :] = chunk(spot).astype(jnp.bfloat16)
                send_pair(step, which, low, pair)
            for step in range(outer):
                spot = pl.ds(pl.multiple_of((block_of(step) + pair_here) * rows, rows), rows)
                full[spot, :] = chunk(spot)
        else:

            @pl.loop(0, width // 128)
            def _(index):
                spot = pl.ds(pl.multiple_of(index * 128, 128), 128)
                value = chunk(spot)
                full[spot, :] = value
                low[spot, :] = value.astype(jnp.bfloat16)

            for step in range(outer):
                send_pair(step, which, low, pair)

    def ring_step(step, which, arrays):
        full, _, pair, ring, sent, total = arrays
        for index in range(pieces):
            spot = pl.ds(index * piece, piece)
            own = pl.ds(pl.multiple_of((block_of(step) + pair_here) * rows + index * piece, piece), piece)
            pair_copies[step, which, index].wait_recv()
            value = full[own, :] + pair[step, spot, :].astype(jnp.float32)
            if step > 0:
                ring_copies[step - 1, which, index].wait_recv()
                value = value + ring[step - 1, spot, :].astype(jnp.float32)
            if step == outer - 1:
                total[spot, :] = value
                continue
            sent[step, spot, :] = value.astype(jnp.bfloat16)
            copy = remote(
                sent.at[step, spot], ring.at[step, spot],
                r_send.at[step, which, index], r_recv.at[step, which, index], onward,
            )
            copy.start()
            ring_copies[step, which, index] = copy

    make_all(0, out_chunk, out_set)
    tile = min(256, seq_len)
    for start in range(0, seq_len, tile):
        spot = pl.ds(start, tile)
        attn_grad[spot, :] = (dot(target[spot, :], out_all[...], 1, 0) * scale).astype(jnp.bfloat16)
    ring_step(0, 0, out_set)
    done = 1
    for head in range(probs.shape[0]):
        base = head * 3 * HEAD_DIM
        query = projected[:, base : base + HEAD_DIM]
        key = projected[:, base + HEAD_DIM : base + 2 * HEAD_DIM]
        value = projected[:, base + 2 * HEAD_DIM : base + 3 * HEAD_DIM]
        key_grad = jnp.zeros((seq_len, HEAD_DIM), jnp.float32)
        value_grad = jnp.zeros((seq_len, HEAD_DIM), jnp.float32)
        for start in range(0, seq_len, tile):
            spot = pl.ds(start, tile)
            grad = attn_grad[spot, head * HEAD_DIM : (head + 1) * HEAD_DIM]
            prob = probs[head, spot, :]
            prob_grad = dot(grad, value, 1, 1)
            inner = jnp.sum(prob * prob_grad, axis=-1, keepdims=True)
            score_grad = (prob * (prob_grad - inner) * score_scale).astype(jnp.bfloat16)
            qkv_grad[spot, base : base + HEAD_DIM] = dot(score_grad, key, 1, 0).astype(jnp.bfloat16)
            key_grad = key_grad + dot(score_grad, query[start : start + tile], 0, 0)
            value_grad = value_grad + dot(prob.astype(jnp.bfloat16), grad, 0, 0)
        qkv_grad[:, base + HEAD_DIM : base + 2 * HEAD_DIM] = key_grad.astype(jnp.bfloat16)
        qkv_grad[:, base + 2 * HEAD_DIM : base + 3 * HEAD_DIM] = value_grad.astype(jnp.bfloat16)
        if done < outer - 1:
            ring_step(done, 0, out_set)
            done += 1
    make_all(1, in_chunk, in_set)
    for step in range(done, outer):
        ring_step(step, 0, out_set)
    for step in range(outer):
        ring_step(step, 1, in_set)
    for copy in pair_copies.values():
        copy.wait_send()
    for copy in ring_copies.values():
        copy.wait_send()


def back_all(dp_size, loss_scale, score_scale, target, attn_rows, out_all, mixed, projected, probs):
    width, out_cols = out_all.shape
    rows = width // dp_size
    in_cols = projected.shape[1]
    seq_len = target.shape[0]
    low = jnp.bfloat16
    outer = dp_size // 2
    both = (in_cols, out_cols)
    return pl.pallas_call(
        functools.partial(back_kernel, dp_size, loss_scale, score_scale),
        out_shape=(
            jax.ShapeDtypeStruct((rows, in_cols), jnp.float32),
            jax.ShapeDtypeStruct((rows, out_cols), jnp.float32),
        ),
        in_specs=[VMEM] * 6,
        out_specs=(VMEM, VMEM),
        scratch_shapes=[pltpu.VMEM((width, cols), jnp.float32) for cols in both]
        + [pltpu.VMEM((width, cols), low) for cols in both]
        + [pltpu.VMEM((outer, rows, cols), low) for _ in range(3) for cols in both]
        + [pltpu.VMEM((seq_len, out_cols), low), pltpu.VMEM((seq_len, in_cols), low)]
        + [pltpu.SemaphoreType.DMA((outer, 2, 4)) for _ in range(4)],
        compiler_params=pltpu.CompilerParams(
            collective_id=2, has_side_effects=True, vmem_limit_bytes=60 * 2**20
        ),
    )(target, attn_rows, out_all, mixed, projected, probs)


def local(dp_size, clean_latents, noise_latents, step_index, labels, class_shift, w_qkv, w_out_t):
    latent_count, part_len, model_width = clean_latents.shape
    score_scale = 1.0 / math.sqrt(HEAD_DIM)
    seq_len = part_len * 4
    loss_scale = 1.0 / math.sqrt(dp_size * latent_count * seq_len)
    step_times, amplitude, amp_rate = time_terms(step_index, model_width)
    offset = lax.dynamic_slice(class_shift, (labels[0], 0), (1, model_width)).astype(jnp.float32)
    cos_t, sin_t = jnp.cos(step_times[0]), jnp.sin(step_times[0])
    row = (1, model_width)
    aux = jnp.concatenate(
        [
            1.0 + amplitude,
            amp_rate,
            offset,
            jnp.broadcast_to(cos_t, row),
            jnp.broadcast_to(sin_t, row),
            jnp.zeros((3, model_width), jnp.float32),
        ]
    )
    clean, noise = clean_latents[0], noise_latents[0]
    mixed_rows, _, _, out_all, projected, probs, attn_rows, blend = gather_all(
        dp_size, score_scale, clean, noise, aux, w_qkv, w_out_t
    )
    partial = lax.dot_general(
        blend, out_all, (((1,), (1,)), ((), ())), preferred_element_type=jnp.float32
    ).astype(jnp.bfloat16)
    target = gather_target(clean, noise, aux, partial)
    return back_all(
        dp_size, loss_scale, score_scale, target, attn_rows, out_all, mixed_rows, projected, probs
    )


def solution(mesh):
    in_specs = (
        P("dp", "tensor", None),
        P("dp", "tensor", None),
        P("dp"),
        P("dp"),
        P(),
        P("dp", "tensor"),
        P("dp", "tensor"),
    )
    out_specs = (P("dp", "tensor"), P("dp", "tensor"))
    step = functools.partial(local, mesh.shape["dp"])
    return jax.shard_map(step, mesh=mesh, in_specs=in_specs, out_specs=out_specs, check_vma=False)
```

```python
import functools
import math

import jax
import jax.numpy as jnp
from jax import lax
from jax.experimental import pallas as pl
from jax.experimental.pallas import tpu as pltpu
from jax.sharding import PartitionSpec as P

HEAD_DIM = 128
STEPS = 1000


norm_eps = 1e-06
target_floor = 0.1


def time_terms(step_index, model_width):
    step_times = 1.4 * (step_index.astype(jnp.float32) + 0.5) / STEPS
    feature_ids = jnp.arange(model_width, dtype=jnp.float32)
    frequency = jnp.exp(-math.log(100.0) * feature_ids / model_width)
    phases = step_times[:, None] * frequency[None, :] + feature_ids[None, :]
    return (step_times, 0.5 * jnp.sin(phases), 0.5 * frequency[None, :] * jnp.cos(phases))


MESH = pl.DeviceIdType.MESH
VMEM = pl.BlockSpec(memory_space=pltpu.VMEM)
HBM = pl.BlockSpec(memory_space=pl.ANY)


def places():
    dp_here, tensor_here = lax.axis_index("dp"), lax.axis_index("tensor")
    sibling = tensor_here + 1 - 2 * lax.rem(tensor_here, 2)
    opposite = lax.rem(tensor_here + 2, 4)
    diagonal = lax.rem(sibling + 2, 4)
    return dp_here, tensor_here, sibling, opposite, diagonal


def greet(devices):
    barrier = pltpu.get_barrier_semaphore()
    for device in devices:
        pl.semaphore_signal(barrier, inc=1, device_id=device, device_id_type=MESH)
    pl.semaphore_wait(barrier, len(devices))


def remote(source, target, send_sem, recv_sem, device):
    return pltpu.make_async_remote_copy(
        src_ref=source,
        dst_ref=target,
        send_sem=send_sem,
        recv_sem=recv_sem,
        device_id=device,
        device_id_type=MESH,
    )


def rows_of(ref, index, count):
    return ref.at[pl.ds(pl.multiple_of(index * count, count), count)]


def dot(left, right, left_dim, right_dim):
    return lax.dot_general(
        left, right, (((left_dim,), (right_dim,)), ((), ())), preferred_element_type=jnp.float32
    )


def gather_kernel(
    dp_size, score_scale, clean, noise, aux, w_qkv, w_out, mixed_all, rate_all, qkv_all, out_all,
    projected, probs, attn_rows, blend, mixed_held, rate_held, qkv_held, projected_rate,
    clean_held, noise_held, mixed, rate, w_send, w_recv, p_send, p_recv, t_send, t_recv, own_sem,
):
    dp_here, tensor_here, sibling, opposite, diagonal = places()
    part = clean.shape[0]
    qkv_rows = w_qkv.shape[0]
    latent_loads = [
        pltpu.make_async_copy(clean, clean_held, own_sem.at[4]),
        pltpu.make_async_copy(noise, noise_held, own_sem.at[5]),
    ]
    for copy in latent_loads:
        copy.start()
    outer = dp_size // 2
    outer_here, pair_here = dp_here // 2, lax.rem(dp_here, 2)
    onward = (lax.rem(outer_here + 1, outer) * 2 + pair_here, tensor_here)
    backward = (lax.rem(outer_here + outer - 1, outer) * 2 + pair_here, tensor_here)
    partner = (outer_here * 2 + 1 - pair_here, tensor_here)
    greet([onward, backward, partner, (dp_here, sibling), (dp_here, opposite)])
    pieces = min(2, qkv_rows // 16)
    piece = qkv_rows // pieces
    ring_copies, pair_copies = {}, {}

    def ring_step(step, which):
        block = lax.rem(outer_here - step + outer, outer) * 2 + pair_here
        held, full = ((w_qkv, qkv_all), (w_out, out_all))[which]
        for index in range(pieces):
            spot = rows_of(full, block * pieces + index, piece)
            source = held.at[pl.ds(index * piece, piece)] if step == 0 else spot
            if step > 0:
                ring_copies[step - 1, which, index].wait_recv()
            if step < outer - 1:
                copy = remote(
                    source, spot, w_send.at[step, which, index], w_recv.at[step, which, index], onward
                )
                copy.start()
                ring_copies[step, which, index] = copy
            copy = remote(source, spot, p_send.at[step, which, index], p_recv.at[step, which, index], partner)
            copy.start()
            pair_copies[step, which, index] = copy

    ring_step(0, 0)
    local_copies = [
        pltpu.make_async_copy(w_qkv, rows_of(qkv_all, dp_here, qkv_rows), own_sem.at[0]),
        pltpu.make_async_copy(w_out, rows_of(out_all, dp_here, qkv_rows), own_sem.at[1]),
    ]
    for copy in local_copies:
        copy.start()
    for copy in latent_loads:
        copy.wait()
    cos_t, sin_t = aux[3:4, :], aux[4:5, :]
    scale_up, amp_rate, offset = aux[0:1, :], aux[1:2, :], aux[2:3, :]

    @pl.loop(0, part // 16)
    def _(index):
        rows = pl.ds(pl.multiple_of(index * 16, 16), 16)
        clean_wide = clean_held[rows, :].astype(jnp.float32)
        noise_wide = noise_held[rows, :].astype(jnp.float32)
        noisy = cos_t * clean_wide + sin_t * noise_wide
        velocity = cos_t * noise_wide - sin_t * clean_wide
        inverse = lax.rsqrt(jnp.mean(noisy * noisy, axis=-1, keepdims=True) + norm_eps)
        cross = jnp.mean(noisy * velocity, axis=-1, keepdims=True)
        normed = noisy * inverse
        normed_rate = velocity * inverse - noisy * (inverse * inverse * inverse * cross)
        mixed[rows, :] = (normed * scale_up + offset).astype(jnp.bfloat16)
        rate[rows, :] = (normed_rate * scale_up + normed * amp_rate).astype(jnp.bfloat16)

    sends, forwards = [], []
    for which, (held, full) in enumerate(((mixed, mixed_all), (rate, rate_all))):
        spot = rows_of(full, tensor_here, part)
        to_opposite = remote(held, spot, t_send.at[which, 0], t_recv.at[which, 0], (dp_here, opposite))
        to_opposite.start()
        to_sibling = remote(held, spot, t_send.at[which, 1], t_recv.at[which, 1], (dp_here, sibling))
        to_sibling.start()
        own = pltpu.make_async_copy(held, spot, own_sem.at[2 + which])
        own.start()
        local_copies.append(own)
        arrived = rows_of(full, opposite, part)
        forward = remote(arrived, arrived, t_send.at[which, 2], t_recv.at[which, 2], (dp_here, sibling))
        sends.append((to_opposite, to_sibling))
        forwards.append(forward)
    for step in range(max(outer - 1, 2)):
        if step + 1 < outer:
            ring_step(step + 1, 0)
        if step < 2:
            sends[step][0].wait_recv()
            forwards[step].start()
    ring_step(0, 1)
    for copy in local_copies:
        copy.wait()
    loads = []
    for which, (full, held) in enumerate(((mixed_all, mixed_held), (rate_all, rate_held))):
        sends[which][1].wait_recv()
        forwards[which].wait_recv()
        load = pltpu.make_async_copy(full, held, own_sem.at[6 + which])
        load.start()
        loads.append(load)
    for (_, which, _), copy in pair_copies.items():
        if which == 0:
            copy.wait_recv()
    load = pltpu.make_async_copy(qkv_all, qkv_held, own_sem.at[8])
    load.start()
    loads.append(load)
    for load in loads:
        load.wait()
    seq_len = mixed_held.shape[0]
    tile = min(256, seq_len)
    for step, (held, result) in enumerate(((mixed_held, projected), (rate_held, projected_rate))):
        for start in range(0, seq_len, tile):
            spot = pl.ds(start, tile)
            result[spot, :] = dot(held[spot, :], qkv_held[...], 1, 0).astype(jnp.bfloat16)
        if step + 1 < outer:
            ring_step(step + 1, 1)
    cos_part, sin_part = aux[3:4, :HEAD_DIM], aux[4:5, :HEAD_DIM]
    done = 3
    for head in range(probs.shape[0]):
        base = head * 3 * HEAD_DIM
        columns = [slice(base + part * HEAD_DIM, base + (part + 1) * HEAD_DIM) for part in range(3)]
        key, key_rate = projected[:, columns[1]], projected_rate[:, columns[1]]
        value, value_rate = projected[:, columns[2]], projected_rate[:, columns[2]]
        here = slice(head * HEAD_DIM, (head + 1) * HEAD_DIM)
        for start in range(0, seq_len, tile):
            spot = pl.ds(start, tile)
            query, query_rate = projected[spot, columns[0]], projected_rate[spot, columns[0]]
            scores = dot(query, key, 1, 1) * score_scale
            score_rate = (dot(query_rate, key, 1, 1) + dot(query, key_rate, 1, 1)) * score_scale
            prob = jnp.exp(scores - jnp.max(scores, axis=-1, keepdims=True))
            prob = prob * (1.0 / jnp.sum(prob, axis=-1, keepdims=True))
            inner = jnp.sum(prob * score_rate, axis=-1, keepdims=True)
            prob_rate = (prob * (score_rate - inner)).astype(jnp.bfloat16)
            probs[head, spot, :] = prob
            prob_low = prob.astype(jnp.bfloat16)
            attn = dot(prob_low, value, 1, 0)
            attn_rate = dot(prob_rate, value, 1, 0) + dot(prob_low, value_rate, 1, 0)
            attn_rows[spot, here] = attn.astype(jnp.bfloat16)
            mix = cos_part * cos_part * attn + cos_part * sin_part * attn_rate
            blend[spot, here] = mix.astype(jnp.bfloat16)
        if done < outer:
            ring_step(done, 1)
            done += 1
    for step in range(done, outer):
        ring_step(step, 1)
    for (to_opposite, to_sibling), forward in zip(sends, forwards):
        to_opposite.wait_send()
        to_sibling.wait_send()
        forward.wait_send()
    for copy in ring_copies.values():
        copy.wait_send()
    for (_, which, _), copy in pair_copies.items():
        copy.wait_send()
        if which == 1:
            copy.wait_recv()


def gather_all(dp_size, score_scale, clean, noise, aux, w_qkv, w_out):
    part, width = clean.shape
    low = jnp.bfloat16
    seq_len, cols, head_cols = 4 * part, w_qkv.shape[1], w_out.shape[1]
    return pl.pallas_call(
        functools.partial(gather_kernel, dp_size, score_scale),
        out_shape=(
            jax.ShapeDtypeStruct((4 * part, width), low),
            jax.ShapeDtypeStruct((4 * part, width), low),
            jax.ShapeDtypeStruct((dp_size * w_qkv.shape[0], w_qkv.shape[1]), low),
            jax.ShapeDtypeStruct((dp_size * w_out.shape[0], w_out.shape[1]), low),
            jax.ShapeDtypeStruct((seq_len, cols), low),
            jax.ShapeDtypeStruct((head_cols // HEAD_DIM, seq_len, seq_len), jnp.float32),
            jax.ShapeDtypeStruct((seq_len, head_cols), low),
            jax.ShapeDtypeStruct((seq_len, head_cols), low),
        ),
        in_specs=[HBM, HBM, VMEM, HBM, HBM],
        out_specs=(HBM,) * 4 + (VMEM,) * 4,
        scratch_shapes=[
            pltpu.VMEM((seq_len, width), low),
            pltpu.VMEM((seq_len, width), low),
            pltpu.VMEM((dp_size * w_qkv.shape[0], cols), low),
            pltpu.VMEM((seq_len, cols), low),
            pltpu.VMEM((part, width), low),
            pltpu.VMEM((part, width), low),
            pltpu.VMEM((part, width), low),
            pltpu.VMEM((part, width), low),
            pltpu.SemaphoreType.DMA((dp_size // 2, 2, 2)),
            pltpu.SemaphoreType.DMA((dp_size // 2, 2, 2)),
            pltpu.SemaphoreType.DMA((dp_size // 2, 2, 2)),
            pltpu.SemaphoreType.DMA((dp_size // 2, 2, 2)),
            pltpu.SemaphoreType.DMA((2, 3)),
            pltpu.SemaphoreType.DMA((2, 3)),
            pltpu.SemaphoreType.DMA((9,)),
        ],
        compiler_params=pltpu.CompilerParams(
            collective_id=0, has_side_effects=True, vmem_limit_bytes=60 * 2**20
        ),
    )(clean, noise, aux, w_qkv, w_out)


PIECES = 8


def target_kernel(
    clean, noise, aux, partial, target_all, first, from_sibling, from_opposite, summed, target,
    load_sem, r_send, r_recv, g_send, g_recv,
):
    dp_here, tensor_here, sibling, opposite, diagonal = places()
    part = clean.shape[0]
    piece = part // PIECES
    greet([(dp_here, sibling), (dp_here, opposite)])

    def block(owner, index):
        return rows_of(partial, owner * PIECES + index, piece)

    def slot(ref, index):
        return ref.at[pl.ds(index * piece, piece)]

    cross, direct, across, loads = [], [], [], []
    for index in range(PIECES):
        copy = remote(
            block(diagonal, index), slot(from_sibling.at[0], index), r_send.at[0, index], r_recv.at[0, index],
            (dp_here, sibling),
        )
        copy.start()
        cross.append(copy)
        load = pltpu.make_async_copy(block(opposite, index), slot(first.at[0], index), load_sem.at[0, index])
        load.start()
        loads.append(load)
    own_loads = []
    for index in range(PIECES):
        copy = remote(
            block(sibling, index), slot(from_sibling.at[1], index), r_send.at[1, index], r_recv.at[1, index],
            (dp_here, sibling),
        )
        copy.start()
        direct.append(copy)
        load = pltpu.make_async_copy(block(tensor_here, index), slot(first.at[1], index), load_sem.at[1, index])
        load.start()
        own_loads.append(load)
    for index in range(PIECES):
        cross[index].wait_recv()
        loads[index].wait()
        rows = pl.ds(index * piece, piece)
        total = first[0, rows, :].astype(jnp.float32) + from_sibling[0, rows, :].astype(jnp.float32)
        summed[rows, :] = total.astype(jnp.bfloat16)
        copy = remote(
            slot(summed, index), slot(from_opposite, index), r_send.at[2, index], r_recv.at[2, index],
            (dp_here, opposite),
        )
        copy.start()
        across.append(copy)
    cos_t, sin_t = aux[3:4, :], aux[4:5, :]
    sends, forwards = [], []

    def spot(owner, index):
        return rows_of(target_all, owner * PIECES + index, piece)

    for index in range(PIECES):
        across[index].wait_recv()
        direct[index].wait_recv()
        own_loads[index].wait()
        rows = pl.ds(index * piece, piece)
        clean_wide = clean[rows, :].astype(jnp.float32)
        noise_wide = noise[rows, :].astype(jnp.float32)
        noisy = cos_t * clean_wide + sin_t * noise_wide
        velocity = cos_t * noise_wide - sin_t * clean_wide
        moved = (
            first[1, rows, :].astype(jnp.float32)
            + from_sibling[1, rows, :].astype(jnp.float32)
            + from_opposite[rows, :].astype(jnp.float32)
        )
        value = -(cos_t * cos_t) * (noisy - velocity) - cos_t * sin_t * (noisy + velocity) - moved
        target[rows, :] = value.astype(jnp.bfloat16)
        held = slot(target, index)
        to_opposite = remote(
            held, spot(tensor_here, index), g_send.at[0, index], g_recv.at[0, index], (dp_here, opposite)
        )
        to_opposite.start()
        to_sibling = remote(
            held, spot(tensor_here, index), g_send.at[1, index], g_recv.at[1, index], (dp_here, sibling)
        )
        to_sibling.start()
        own = pltpu.make_async_copy(held, spot(tensor_here, index), load_sem.at[2, index])
        own.start()
        forward = remote(
            spot(opposite, index), spot(opposite, index), g_send.at[2, index], g_recv.at[2, index], (dp_here, sibling)
        )
        sends.append((to_opposite, to_sibling, own, forward))
    for to_opposite, to_sibling, own, forward in sends:
        to_opposite.wait_recv()
        forward.start()
    for index, (to_opposite, to_sibling, own, forward) in enumerate(sends):
        to_opposite.wait_send()
        to_sibling.wait()
        own.wait()
        forward.wait()
        cross[index].wait_send()
        direct[index].wait_send()
        across[index].wait_send()


def gather_target(clean, noise, aux, partial):
    part, width = clean.shape
    low = jnp.bfloat16
    return pl.pallas_call(
        target_kernel,
        out_shape=jax.ShapeDtypeStruct((4 * part, width), low),
        in_specs=[VMEM, VMEM, VMEM, HBM],
        out_specs=HBM,
        scratch_shapes=[
            pltpu.VMEM((2, part, width), low),
            pltpu.VMEM((2, part, width), low),
            pltpu.VMEM((part, width), low),
            pltpu.VMEM((part, width), low),
            pltpu.VMEM((part, width), low),
            pltpu.SemaphoreType.DMA((3, PIECES)),
            pltpu.SemaphoreType.DMA((3, PIECES)),
            pltpu.SemaphoreType.DMA((3, PIECES)),
            pltpu.SemaphoreType.DMA((3, PIECES)),
            pltpu.SemaphoreType.DMA((3, PIECES)),
        ],
        compiler_params=pltpu.CompilerParams(
            collective_id=1, has_side_effects=True, vmem_limit_bytes=32 * 2**20
        ),
    )(clean, noise, aux, partial)


def back_kernel(
    dp_size, loss_scale, score_scale, target, attn_rows, out_all, mixed, projected, probs, in_sum, out_sum,
    in_full, out_full, in_low, out_low, in_pair, out_pair, in_ring, out_ring, in_sent, out_sent,
    attn_grad, qkv_grad, p_send, p_recv, r_send, r_recv,
):
    dp_here, tensor_here, _, _, _ = places()
    rows = in_sum.shape[0]
    seq_len, width = target.shape
    outer = dp_size // 2
    outer_here, pair_here = dp_here // 2, lax.rem(dp_here, 2)
    onward = (lax.rem(outer_here + 1, outer) * 2 + pair_here, tensor_here)
    backward = (lax.rem(outer_here + outer - 1, outer) * 2 + pair_here, tensor_here)
    partner = (outer_here * 2 + 1 - pair_here, tensor_here)
    greet([onward, backward, partner])
    pieces = min(4, rows // 16)
    piece = rows // pieces
    out_set = (out_full, out_low, out_pair, out_ring, out_sent, out_sum)
    in_set = (in_full, in_low, in_pair, in_ring, in_sent, in_sum)
    pair_copies, ring_copies = {}, {}

    def squares(index, held):
        spot = pl.ds(pl.multiple_of(index * 16, 16), 16)
        value = target[spot, :].astype(jnp.float32)
        return held + value * value

    total = lax.fori_loop(0, seq_len // 16, squares, jnp.zeros((16, width), jnp.float32))
    total = jnp.sum(jnp.sum(total, axis=0, keepdims=True), axis=1, keepdims=True)
    scale = -loss_scale / (jnp.sqrt(total / (seq_len * width)) + target_floor)

    def out_chunk(spot):
        return dot(target[:, spot], attn_rows[...], 0, 0) * scale

    def in_chunk(spot):
        return dot(mixed[:, spot], qkv_grad[...], 0, 0)

    def block_of(step):
        return lax.rem(outer_here - step - 1 + outer, outer) * 2

    def send_pair(step, which, low, pair):
        for index in range(pieces):
            copy = remote(
                rows_of(low, (block_of(step) + 1 - pair_here) * pieces + index, piece),
                pair.at[step, pl.ds(index * piece, piece)],
                p_send.at[step, which, index], p_recv.at[step, which, index], partner,
            )
            copy.start()
            pair_copies[step, which, index] = copy

    def make_all(which, chunk, arrays):
        full, low, pair = arrays[:3]
        if rows % 128 == 0:
            for step in range(outer):
                spot = pl.ds(pl.multiple_of((block_of(step) + 1 - pair_here) * rows, rows), rows)
                low[spot, :] = chunk(spot).astype(jnp.bfloat16)
                send_pair(step, which, low, pair)
            for step in range(outer):
                spot = pl.ds(pl.multiple_of((block_of(step) + pair_here) * rows, rows), rows)
                full[spot, :] = chunk(spot)
        else:

            @pl.loop(0, width // 128)
            def _(index):
                spot = pl.ds(pl.multiple_of(index * 128, 128), 128)
                value = chunk(spot)
                full[spot, :] = value
                low[spot, :] = value.astype(jnp.bfloat16)

            for step in range(outer):
                send_pair(step, which, low, pair)

    def ring_step(step, which, arrays):
        full, _, pair, ring, sent, total = arrays
        for index in range(pieces):
            spot = pl.ds(index * piece, piece)
            own = pl.ds(pl.multiple_of((block_of(step) + pair_here) * rows + index * piece, piece), piece)
            pair_copies[step, which, index].wait_recv()
            value = full[own, :] + pair[step, spot, :].astype(jnp.float32)
            if step > 0:
                ring_copies[step - 1, which, index].wait_recv()
                value = value + ring[step - 1, spot, :].astype(jnp.float32)
            if step == outer - 1:
                total[spot, :] = value
                continue
            sent[step, spot, :] = value.astype(jnp.bfloat16)
            copy = remote(
                sent.at[step, spot], ring.at[step, spot],
                r_send.at[step, which, index], r_recv.at[step, which, index], onward,
            )
            copy.start()
            ring_copies[step, which, index] = copy

    make_all(0, out_chunk, out_set)
    tile = min(256, seq_len)
    for start in range(0, seq_len, tile):
        spot = pl.ds(start, tile)
        attn_grad[spot, :] = (dot(target[spot, :], out_all[...], 1, 0) * scale).astype(jnp.bfloat16)
    ring_step(0, 0, out_set)
    done = 1
    for head in range(probs.shape[0]):
        base = head * 3 * HEAD_DIM
        query = projected[:, base : base + HEAD_DIM]
        key = projected[:, base + HEAD_DIM : base + 2 * HEAD_DIM]
        value = projected[:, base + 2 * HEAD_DIM : base + 3 * HEAD_DIM]
        key_grad = jnp.zeros((seq_len, HEAD_DIM), jnp.float32)
        value_grad = jnp.zeros((seq_len, HEAD_DIM), jnp.float32)
        for start in range(0, seq_len, tile):
            spot = pl.ds(start, tile)
            grad = attn_grad[spot, head * HEAD_DIM : (head + 1) * HEAD_DIM]
            prob = probs[head, spot, :]
            prob_grad = dot(grad, value, 1, 1)
            inner = jnp.sum(prob * prob_grad, axis=-1, keepdims=True)
            score_grad = (prob * (prob_grad - inner) * score_scale).astype(jnp.bfloat16)
            qkv_grad[spot, base : base + HEAD_DIM] = dot(score_grad, key, 1, 0).astype(jnp.bfloat16)
            key_grad = key_grad + dot(score_grad, query[start : start + tile], 0, 0)
            value_grad = value_grad + dot(prob.astype(jnp.bfloat16), grad, 0, 0)
        qkv_grad[:, base + HEAD_DIM : base + 2 * HEAD_DIM] = key_grad.astype(jnp.bfloat16)
        qkv_grad[:, base + 2 * HEAD_DIM : base + 3 * HEAD_DIM] = value_grad.astype(jnp.bfloat16)
        if done < outer - 1:
            ring_step(done, 0, out_set)
            done += 1
    make_all(1, in_chunk, in_set)
    for step in range(done, outer):
        ring_step(step, 0, out_set)
    for step in range(outer):
        ring_step(step, 1, in_set)
    for copy in pair_copies.values():
        copy.wait_send()
    for copy in ring_copies.values():
        copy.wait_send()


def back_all(dp_size, loss_scale, score_scale, target, attn_rows, out_all, mixed, projected, probs):
    width, out_cols = out_all.shape
    rows = width // dp_size
    in_cols = projected.shape[1]
    seq_len = target.shape[0]
    low = jnp.bfloat16
    outer = dp_size // 2
    both = (in_cols, out_cols)
    return pl.pallas_call(
        functools.partial(back_kernel, dp_size, loss_scale, score_scale),
        out_shape=(
            jax.ShapeDtypeStruct((rows, in_cols), jnp.float32),
            jax.ShapeDtypeStruct((rows, out_cols), jnp.float32),
        ),
        in_specs=[VMEM] * 6,
        out_specs=(VMEM, VMEM),
        scratch_shapes=[pltpu.VMEM((width, cols), jnp.float32) for cols in both]
        + [pltpu.VMEM((width, cols), low) for cols in both]
        + [pltpu.VMEM((outer, rows, cols), low) for _ in range(3) for cols in both]
        + [pltpu.VMEM((seq_len, out_cols), low), pltpu.VMEM((seq_len, in_cols), low)]
        + [pltpu.SemaphoreType.DMA((outer, 2, 4)) for _ in range(4)],
        compiler_params=pltpu.CompilerParams(
            collective_id=2, has_side_effects=True, vmem_limit_bytes=36 * 2**20
        ),
    )(target, attn_rows, out_all, mixed, projected, probs)


def local(dp_size, clean_latents, noise_latents, step_index, labels, class_shift, w_qkv, w_out_t):
    latent_count, part_len, model_width = clean_latents.shape
    score_scale = 1.0 / math.sqrt(HEAD_DIM)
    seq_len = part_len * 4
    loss_scale = 1.0 / math.sqrt(dp_size * latent_count * seq_len)
    step_times, amplitude, amp_rate = time_terms(step_index, model_width)
    offset = lax.dynamic_slice(class_shift, (labels[0], 0), (1, model_width)).astype(jnp.float32)
    cos_t, sin_t = jnp.cos(step_times[0]), jnp.sin(step_times[0])
    row = (1, model_width)
    aux = jnp.concatenate(
        [
            1.0 + amplitude,
            amp_rate,
            offset,
            jnp.broadcast_to(cos_t, row),
            jnp.broadcast_to(sin_t, row),
            jnp.zeros((3, model_width), jnp.float32),
        ]
    )
    clean, noise = clean_latents[0], noise_latents[0]
    mixed_rows, _, _, out_all, projected, probs, attn_rows, blend = gather_all(
        dp_size, score_scale, clean, noise, aux, w_qkv, w_out_t
    )
    partial = lax.dot_general(
        blend, out_all, (((1,), (1,)), ((), ())), preferred_element_type=jnp.float32
    ).astype(jnp.bfloat16)
    target = gather_target(clean, noise, aux, partial)
    return back_all(
        dp_size, loss_scale, score_scale, target, attn_rows, out_all, mixed_rows, projected, probs
    )


def solution(mesh):
    in_specs = (
        P("dp", "tensor", None),
        P("dp", "tensor", None),
        P("dp"),
        P("dp"),
        P(),
        P("dp", "tensor"),
        P("dp", "tensor"),
    )
    out_specs = (P("dp", "tensor"), P("dp", "tensor"))
    step = functools.partial(local, mesh.shape["dp"])
    return jax.shard_map(step, mesh=mesh, in_specs=in_specs, out_specs=out_specs, check_vma=False)
```

```python
import functools
import math

import jax
import jax.numpy as jnp
from jax import lax
from jax.experimental import pallas as pl
from jax.experimental.pallas import tpu as pltpu
from jax.sharding import PartitionSpec as P

HEAD_DIM = 128
STEPS = 1000


norm_eps = 1e-06
target_floor = 0.1


def time_terms(step_index, model_width):
    step_times = 1.4 * (step_index.astype(jnp.float32) + 0.5) / STEPS
    feature_ids = jnp.arange(model_width, dtype=jnp.float32)
    frequency = jnp.exp(-math.log(100.0) * feature_ids / model_width)
    phases = step_times[:, None] * frequency[None, :] + feature_ids[None, :]
    return (step_times, 0.5 * jnp.sin(phases), 0.5 * frequency[None, :] * jnp.cos(phases))


MESH = pl.DeviceIdType.MESH
VMEM = pl.BlockSpec(memory_space=pltpu.VMEM)
HBM = pl.BlockSpec(memory_space=pl.ANY)


def places():
    dp_here, tensor_here = lax.axis_index("dp"), lax.axis_index("tensor")
    sibling = tensor_here + 1 - 2 * lax.rem(tensor_here, 2)
    opposite = lax.rem(tensor_here + 2, 4)
    diagonal = lax.rem(sibling + 2, 4)
    return dp_here, tensor_here, sibling, opposite, diagonal


def greet(devices):
    barrier = pltpu.get_barrier_semaphore()
    for device in devices:
        pl.semaphore_signal(barrier, inc=1, device_id=device, device_id_type=MESH)
    pl.semaphore_wait(barrier, len(devices))


def remote(source, target, send_sem, recv_sem, device):
    return pltpu.make_async_remote_copy(
        src_ref=source,
        dst_ref=target,
        send_sem=send_sem,
        recv_sem=recv_sem,
        device_id=device,
        device_id_type=MESH,
    )


def rows_of(ref, index, count):
    return ref.at[pl.ds(pl.multiple_of(index * count, count), count)]


def dot(left, right, left_dim, right_dim):
    return lax.dot_general(
        left, right, (((left_dim,), (right_dim,)), ((), ())), preferred_element_type=jnp.float32
    )


def gather_kernel(
    dp_size, score_scale, clean, noise, aux, w_qkv, w_out, mixed_all, rate_all, qkv_all, out_all,
    projected, probs, attn_rows, blend, mixed_held, rate_held, qkv_held, projected_rate,
    clean_held, noise_held, mixed, rate, w_send, w_recv, p_send, p_recv, t_send, t_recv, own_sem,
):
    dp_here, tensor_here, sibling, opposite, diagonal = places()
    part = clean.shape[0]
    qkv_rows = w_qkv.shape[0]
    latent_loads = [
        pltpu.make_async_copy(clean, clean_held, own_sem.at[4]),
        pltpu.make_async_copy(noise, noise_held, own_sem.at[5]),
    ]
    for copy in latent_loads:
        copy.start()
    outer = dp_size // 2
    outer_here, pair_here = dp_here // 2, lax.rem(dp_here, 2)
    onward = (lax.rem(outer_here + 1, outer) * 2 + pair_here, tensor_here)
    backward = (lax.rem(outer_here + outer - 1, outer) * 2 + pair_here, tensor_here)
    partner = (outer_here * 2 + 1 - pair_here, tensor_here)
    greet([onward, backward, partner, (dp_here, sibling), (dp_here, opposite)])
    pieces = min(4, qkv_rows // 16)
    piece = qkv_rows // pieces
    ring_copies, pair_copies = {}, {}

    def ring_step(step, which):
        block = lax.rem(outer_here - step + outer, outer) * 2 + pair_here
        held, full = ((w_qkv, qkv_all), (w_out, out_all))[which]
        for index in range(pieces):
            spot = rows_of(full, block * pieces + index, piece)
            source = held.at[pl.ds(index * piece, piece)] if step == 0 else spot
            if step > 0:
                ring_copies[step - 1, which, index].wait_recv()
            if step < outer - 1:
                copy = remote(
                    source, spot, w_send.at[step, which, index], w_recv.at[step, which, index], onward
                )
                copy.start()
                ring_copies[step, which, index] = copy
            copy = remote(source, spot, p_send.at[step, which, index], p_recv.at[step, which, index], partner)
            copy.start()
            pair_copies[step, which, index] = copy

    ring_step(0, 0)
    local_copies = [
        pltpu.make_async_copy(w_qkv, rows_of(qkv_all, dp_here, qkv_rows), own_sem.at[0]),
        pltpu.make_async_copy(w_out, rows_of(out_all, dp_here, qkv_rows), own_sem.at[1]),
    ]
    for copy in local_copies:
        copy.start()
    for copy in latent_loads:
        copy.wait()
    cos_t, sin_t = aux[3:4, :], aux[4:5, :]
    scale_up, amp_rate, offset = aux[0:1, :], aux[1:2, :], aux[2:3, :]

    @pl.loop(0, part // 16)
    def _(index):
        rows = pl.ds(pl.multiple_of(index * 16, 16), 16)
        clean_wide = clean_held[rows, :].astype(jnp.float32)
        noise_wide = noise_held[rows, :].astype(jnp.float32)
        noisy = cos_t * clean_wide + sin_t * noise_wide
        velocity = cos_t * noise_wide - sin_t * clean_wide
        inverse = lax.rsqrt(jnp.mean(noisy * noisy, axis=-1, keepdims=True) + norm_eps)
        cross = jnp.mean(noisy * velocity, axis=-1, keepdims=True)
        normed = noisy * inverse
        normed_rate = velocity * inverse - noisy * (inverse * inverse * inverse * cross)
        mixed[rows, :] = (normed * scale_up + offset).astype(jnp.bfloat16)
        rate[rows, :] = (normed_rate * scale_up + normed * amp_rate).astype(jnp.bfloat16)

    sends, forwards = [], []
    for which, (held, full) in enumerate(((mixed, mixed_all), (rate, rate_all))):
        spot = rows_of(full, tensor_here, part)
        to_opposite = remote(held, spot, t_send.at[which, 0], t_recv.at[which, 0], (dp_here, opposite))
        to_opposite.start()
        to_sibling = remote(held, spot, t_send.at[which, 1], t_recv.at[which, 1], (dp_here, sibling))
        to_sibling.start()
        own = pltpu.make_async_copy(held, spot, own_sem.at[2 + which])
        own.start()
        local_copies.append(own)
        arrived = rows_of(full, opposite, part)
        forward = remote(arrived, arrived, t_send.at[which, 2], t_recv.at[which, 2], (dp_here, sibling))
        sends.append((to_opposite, to_sibling))
        forwards.append(forward)
    for step in range(max(outer - 1, 2)):
        if step + 1 < outer:
            ring_step(step + 1, 0)
        if step < 2:
            sends[step][0].wait_recv()
            forwards[step].start()
    ring_step(0, 1)
    for copy in local_copies:
        copy.wait()
    loads = []
    for which, (full, held) in enumerate(((mixed_all, mixed_held), (rate_all, rate_held))):
        sends[which][1].wait_recv()
        forwards[which].wait_recv()
        load = pltpu.make_async_copy(full, held, own_sem.at[6 + which])
        load.start()
        loads.append(load)
    for (_, which, _), copy in pair_copies.items():
        if which == 0:
            copy.wait_recv()
    load = pltpu.make_async_copy(qkv_all, qkv_held, own_sem.at[8])
    load.start()
    loads.append(load)
    for load in loads:
        load.wait()
    seq_len = mixed_held.shape[0]
    tile = min(256, seq_len)
    for step, (held, result) in enumerate(((mixed_held, projected), (rate_held, projected_rate))):
        for start in range(0, seq_len, tile):
            spot = pl.ds(start, tile)
            result[spot, :] = dot(held[spot, :], qkv_held[...], 1, 0).astype(jnp.bfloat16)
        if step + 1 < outer:
            ring_step(step + 1, 1)
    cos_part, sin_part = aux[3:4, :HEAD_DIM], aux[4:5, :HEAD_DIM]
    done = 3
    for head in range(probs.shape[0]):
        base = head * 3 * HEAD_DIM
        columns = [slice(base + part * HEAD_DIM, base + (part + 1) * HEAD_DIM) for part in range(3)]
        key, key_rate = projected[:, columns[1]], projected_rate[:, columns[1]]
        value, value_rate = projected[:, columns[2]], projected_rate[:, columns[2]]
        here = slice(head * HEAD_DIM, (head + 1) * HEAD_DIM)
        for start in range(0, seq_len, tile):
            spot = pl.ds(start, tile)
            query, query_rate = projected[spot, columns[0]], projected_rate[spot, columns[0]]
            scores = dot(query, key, 1, 1) * score_scale
            score_rate = (dot(query_rate, key, 1, 1) + dot(query, key_rate, 1, 1)) * score_scale
            prob = jnp.exp(scores - jnp.max(scores, axis=-1, keepdims=True))
            prob = prob * (1.0 / jnp.sum(prob, axis=-1, keepdims=True))
            inner = jnp.sum(prob * score_rate, axis=-1, keepdims=True)
            prob_rate = (prob * (score_rate - inner)).astype(jnp.bfloat16)
            probs[head, spot, :] = prob
            prob_low = prob.astype(jnp.bfloat16)
            attn = dot(prob_low, value, 1, 0)
            attn_rate = dot(prob_rate, value, 1, 0) + dot(prob_low, value_rate, 1, 0)
            attn_rows[spot, here] = attn.astype(jnp.bfloat16)
            mix = cos_part * cos_part * attn + cos_part * sin_part * attn_rate
            blend[spot, here] = mix.astype(jnp.bfloat16)
        if done < outer:
            ring_step(done, 1)
            done += 1
    for step in range(done, outer):
        ring_step(step, 1)
    for (to_opposite, to_sibling), forward in zip(sends, forwards):
        to_opposite.wait_send()
        to_sibling.wait_send()
        forward.wait_send()
    for copy in ring_copies.values():
        copy.wait_send()
    for (_, which, _), copy in pair_copies.items():
        copy.wait_send()
        if which == 1:
            copy.wait_recv()


def gather_all(dp_size, score_scale, clean, noise, aux, w_qkv, w_out):
    part, width = clean.shape
    low = jnp.bfloat16
    seq_len, cols, head_cols = 4 * part, w_qkv.shape[1], w_out.shape[1]
    return pl.pallas_call(
        functools.partial(gather_kernel, dp_size, score_scale),
        out_shape=(
            jax.ShapeDtypeStruct((4 * part, width), low),
            jax.ShapeDtypeStruct((4 * part, width), low),
            jax.ShapeDtypeStruct((dp_size * w_qkv.shape[0], w_qkv.shape[1]), low),
            jax.ShapeDtypeStruct((dp_size * w_out.shape[0], w_out.shape[1]), low),
            jax.ShapeDtypeStruct((seq_len, cols), low),
            jax.ShapeDtypeStruct((head_cols // HEAD_DIM, seq_len, seq_len), jnp.float32),
            jax.ShapeDtypeStruct((seq_len, head_cols), low),
            jax.ShapeDtypeStruct((seq_len, head_cols), low),
        ),
        in_specs=[HBM, HBM, VMEM, HBM, HBM],
        out_specs=(HBM,) * 4 + (VMEM,) * 4,
        scratch_shapes=[
            pltpu.VMEM((seq_len, width), low),
            pltpu.VMEM((seq_len, width), low),
            pltpu.VMEM((dp_size * w_qkv.shape[0], cols), low),
            pltpu.VMEM((seq_len, cols), low),
            pltpu.VMEM((part, width), low),
            pltpu.VMEM((part, width), low),
            pltpu.VMEM((part, width), low),
            pltpu.VMEM((part, width), low),
            pltpu.SemaphoreType.DMA((dp_size // 2, 2, 4)),
            pltpu.SemaphoreType.DMA((dp_size // 2, 2, 4)),
            pltpu.SemaphoreType.DMA((dp_size // 2, 2, 4)),
            pltpu.SemaphoreType.DMA((dp_size // 2, 2, 4)),
            pltpu.SemaphoreType.DMA((2, 3)),
            pltpu.SemaphoreType.DMA((2, 3)),
            pltpu.SemaphoreType.DMA((9,)),
        ],
        compiler_params=pltpu.CompilerParams(
            collective_id=0, has_side_effects=True, vmem_limit_bytes=60 * 2**20
        ),
    )(clean, noise, aux, w_qkv, w_out)


PIECES = 4


def target_kernel(
    clean, noise, aux, partial, target_all, first, from_sibling, from_opposite, summed, target,
    load_sem, r_send, r_recv, g_send, g_recv,
):
    dp_here, tensor_here, sibling, opposite, diagonal = places()
    part = clean.shape[0]
    piece = part // PIECES
    greet([(dp_here, sibling), (dp_here, opposite)])

    def block(owner, index):
        return rows_of(partial, owner * PIECES + index, piece)

    def slot(ref, index):
        return ref.at[pl.ds(index * piece, piece)]

    cross, direct, across, loads = [], [], [], []
    for index in range(PIECES):
        copy = remote(
            block(diagonal, index), slot(from_sibling.at[0], index), r_send.at[0, index], r_recv.at[0, index],
            (dp_here, sibling),
        )
        copy.start()
        cross.append(copy)
        load = pltpu.make_async_copy(block(opposite, index), slot(first.at[0], index), load_sem.at[0, index])
        load.start()
        loads.append(load)
    own_loads = []
    for index in range(PIECES):
        copy = remote(
            block(sibling, index), slot(from_sibling.at[1], index), r_send.at[1, index], r_recv.at[1, index],
            (dp_here, sibling),
        )
        copy.start()
        direct.append(copy)
        load = pltpu.make_async_copy(block(tensor_here, index), slot(first.at[1], index), load_sem.at[1, index])
        load.start()
        own_loads.append(load)
    for index in range(PIECES):
        cross[index].wait_recv()
        loads[index].wait()
        rows = pl.ds(index * piece, piece)
        total = first[0, rows, :].astype(jnp.float32) + from_sibling[0, rows, :].astype(jnp.float32)
        summed[rows, :] = total.astype(jnp.bfloat16)
        copy = remote(
            slot(summed, index), slot(from_opposite, index), r_send.at[2, index], r_recv.at[2, index],
            (dp_here, opposite),
        )
        copy.start()
        across.append(copy)
    cos_t, sin_t = aux[3:4, :], aux[4:5, :]
    sends, forwards = [], []

    def spot(owner, index):
        return rows_of(target_all, owner * PIECES + index, piece)

    for index in range(PIECES):
        across[index].wait_recv()
        direct[index].wait_recv()
        own_loads[index].wait()
        rows = pl.ds(index * piece, piece)
        clean_wide = clean[rows, :].astype(jnp.float32)
        noise_wide = noise[rows, :].astype(jnp.float32)
        noisy = cos_t * clean_wide + sin_t * noise_wide
        velocity = cos_t * noise_wide - sin_t * clean_wide
        moved = (
            first[1, rows, :].astype(jnp.float32)
            + from_sibling[1, rows, :].astype(jnp.float32)
            + from_opposite[rows, :].astype(jnp.float32)
        )
        value = -(cos_t * cos_t) * (noisy - velocity) - cos_t * sin_t * (noisy + velocity) - moved
        target[rows, :] = value.astype(jnp.bfloat16)
        held = slot(target, index)
        to_opposite = remote(
            held, spot(tensor_here, index), g_send.at[0, index], g_recv.at[0, index], (dp_here, opposite)
        )
        to_opposite.start()
        to_sibling = remote(
            held, spot(tensor_here, index), g_send.at[1, index], g_recv.at[1, index], (dp_here, sibling)
        )
        to_sibling.start()
        own = pltpu.make_async_copy(held, spot(tensor_here, index), load_sem.at[2, index])
        own.start()
        forward = remote(
            spot(opposite, index), spot(opposite, index), g_send.at[2, index], g_recv.at[2, index], (dp_here, sibling)
        )
        sends.append((to_opposite, to_sibling, own, forward))
    for to_opposite, to_sibling, own, forward in sends:
        to_opposite.wait_recv()
        forward.start()
    for index, (to_opposite, to_sibling, own, forward) in enumerate(sends):
        to_opposite.wait_send()
        to_sibling.wait()
        own.wait()
        forward.wait()
        cross[index].wait_send()
        direct[index].wait_send()
        across[index].wait_send()


def gather_target(clean, noise, aux, partial):
    part, width = clean.shape
    low = jnp.bfloat16
    return pl.pallas_call(
        target_kernel,
        out_shape=jax.ShapeDtypeStruct((4 * part, width), low),
        in_specs=[VMEM, VMEM, VMEM, HBM],
        out_specs=HBM,
        scratch_shapes=[
            pltpu.VMEM((2, part, width), low),
            pltpu.VMEM((2, part, width), low),
            pltpu.VMEM((part, width), low),
            pltpu.VMEM((part, width), low),
            pltpu.VMEM((part, width), low),
            pltpu.SemaphoreType.DMA((3, PIECES)),
            pltpu.SemaphoreType.DMA((3, PIECES)),
            pltpu.SemaphoreType.DMA((3, PIECES)),
            pltpu.SemaphoreType.DMA((3, PIECES)),
            pltpu.SemaphoreType.DMA((3, PIECES)),
        ],
        compiler_params=pltpu.CompilerParams(
            collective_id=1, has_side_effects=True, vmem_limit_bytes=32 * 2**20
        ),
    )(clean, noise, aux, partial)


def back_kernel(
    dp_size, loss_scale, score_scale, target, attn_rows, out_all, mixed, projected, probs, in_sum, out_sum,
    in_full, out_full, in_low, out_low, in_pair, out_pair, in_ring, out_ring, in_sent, out_sent,
    attn_grad, qkv_grad, p_send, p_recv, r_send, r_recv,
):
    dp_here, tensor_here, _, _, _ = places()
    rows = in_sum.shape[0]
    seq_len, width = target.shape
    outer = dp_size // 2
    outer_here, pair_here = dp_here // 2, lax.rem(dp_here, 2)
    onward = (lax.rem(outer_here + 1, outer) * 2 + pair_here, tensor_here)
    backward = (lax.rem(outer_here + outer - 1, outer) * 2 + pair_here, tensor_here)
    partner = (outer_here * 2 + 1 - pair_here, tensor_here)
    greet([onward, backward, partner])
    pieces = min(4, rows // 16)
    piece = rows // pieces
    out_set = (out_full, out_low, out_pair, out_ring, out_sent, out_sum)
    in_set = (in_full, in_low, in_pair, in_ring, in_sent, in_sum)
    pair_copies, ring_copies = {}, {}

    def squares(index, held):
        spot = pl.ds(pl.multiple_of(index * 16, 16), 16)
        value = target[spot, :].astype(jnp.float32)
        return held + value * value

    total = lax.fori_loop(0, seq_len // 16, squares, jnp.zeros((16, width), jnp.float32))
    total = jnp.sum(jnp.sum(total, axis=0, keepdims=True), axis=1, keepdims=True)
    scale = -loss_scale / (jnp.sqrt(total / (seq_len * width)) + target_floor)

    def out_chunk(spot):
        return dot(target[:, spot], attn_rows[...], 0, 0) * scale

    def in_chunk(spot):
        return dot(mixed[:, spot], qkv_grad[...], 0, 0)

    def block_of(step):
        return lax.rem(outer_here - step - 1 + outer, outer) * 2

    def send_pair(step, which, low, pair):
        for index in range(pieces):
            copy = remote(
                rows_of(low, (block_of(step) + 1 - pair_here) * pieces + index, piece),
                pair.at[step, pl.ds(index * piece, piece)],
                p_send.at[step, which, index], p_recv.at[step, which, index], partner,
            )
            copy.start()
            pair_copies[step, which, index] = copy

    def make_all(which, chunk, arrays):
        full, low, pair = arrays[:3]
        if rows % 128 == 0:
            for step in range(outer):
                spot = pl.ds(pl.multiple_of((block_of(step) + 1 - pair_here) * rows, rows), rows)
                low[spot, :] = chunk(spot).astype(jnp.bfloat16)
                send_pair(step, which, low, pair)
            for step in range(outer):
                spot = pl.ds(pl.multiple_of((block_of(step) + pair_here) * rows, rows), rows)
                full[spot, :] = chunk(spot)
        else:

            @pl.loop(0, width // 128)
            def _(index):
                spot = pl.ds(pl.multiple_of(index * 128, 128), 128)
                value = chunk(spot)
                full[spot, :] = value
                low[spot, :] = value.astype(jnp.bfloat16)

            for step in range(outer):
                send_pair(step, which, low, pair)

    def ring_step(step, which, arrays):
        full, _, pair, ring, sent, total = arrays
        for index in range(pieces):
            spot = pl.ds(index * piece, piece)
            own = pl.ds(pl.multiple_of((block_of(step) + pair_here) * rows + index * piece, piece), piece)
            pair_copies[step, which, index].wait_recv()
            value = full[own, :] + pair[step, spot, :].astype(jnp.float32)
            if step > 0:
                ring_copies[step - 1, which, index].wait_recv()
                value = value + ring[step - 1, spot, :].astype(jnp.float32)
            if step == outer - 1:
                total[spot, :] = value
                continue
            sent[step, spot, :] = value.astype(jnp.bfloat16)
            copy = remote(
                sent.at[step, spot], ring.at[step, spot],
                r_send.at[step, which, index], r_recv.at[step, which, index], onward,
            )
            copy.start()
            ring_copies[step, which, index] = copy

    make_all(0, out_chunk, out_set)
    tile = min(256, seq_len)
    for start in range(0, seq_len, tile):
        spot = pl.ds(start, tile)
        attn_grad[spot, :] = (dot(target[spot, :], out_all[...], 1, 0) * scale).astype(jnp.bfloat16)
    ring_step(0, 0, out_set)
    done = 1
    for head in range(probs.shape[0]):
        base = head * 3 * HEAD_DIM
        query = projected[:, base : base + HEAD_DIM]
        key = projected[:, base + HEAD_DIM : base + 2 * HEAD_DIM]
        value = projected[:, base + 2 * HEAD_DIM : base + 3 * HEAD_DIM]
        key_grad = jnp.zeros((seq_len, HEAD_DIM), jnp.float32)
        value_grad = jnp.zeros((seq_len, HEAD_DIM), jnp.float32)
        for start in range(0, seq_len, tile):
            spot = pl.ds(start, tile)
            grad = attn_grad[spot, head * HEAD_DIM : (head + 1) * HEAD_DIM]
            prob = probs[head, spot, :]
            prob_grad = dot(grad, value, 1, 1)
            inner = jnp.sum(prob * prob_grad, axis=-1, keepdims=True)
            score_grad = (prob * (prob_grad - inner) * score_scale).astype(jnp.bfloat16)
            qkv_grad[spot, base : base + HEAD_DIM] = dot(score_grad, key, 1, 0).astype(jnp.bfloat16)
            key_grad = key_grad + dot(score_grad, query[start : start + tile], 0, 0)
            value_grad = value_grad + dot(prob.astype(jnp.bfloat16), grad, 0, 0)
        qkv_grad[:, base + HEAD_DIM : base + 2 * HEAD_DIM] = key_grad.astype(jnp.bfloat16)
        qkv_grad[:, base + 2 * HEAD_DIM : base + 3 * HEAD_DIM] = value_grad.astype(jnp.bfloat16)
        if done < outer - 1:
            ring_step(done, 0, out_set)
            done += 1
    make_all(1, in_chunk, in_set)
    for step in range(done, outer):
        ring_step(step, 0, out_set)
    for step in range(outer):
        ring_step(step, 1, in_set)
    for copy in pair_copies.values():
        copy.wait_send()
    for copy in ring_copies.values():
        copy.wait_send()


def back_all(dp_size, loss_scale, score_scale, target, attn_rows, out_all, mixed, projected, probs):
    width, out_cols = out_all.shape
    rows = width // dp_size
    in_cols = projected.shape[1]
    seq_len = target.shape[0]
    low = jnp.bfloat16
    outer = dp_size // 2
    both = (in_cols, out_cols)
    return pl.pallas_call(
        functools.partial(back_kernel, dp_size, loss_scale, score_scale),
        out_shape=(
            jax.ShapeDtypeStruct((rows, in_cols), jnp.float32),
            jax.ShapeDtypeStruct((rows, out_cols), jnp.float32),
        ),
        in_specs=[VMEM] * 6,
        out_specs=(VMEM, VMEM),
        scratch_shapes=[pltpu.VMEM((width, cols), jnp.float32) for cols in both]
        + [pltpu.VMEM((width, cols), low) for cols in both]
        + [pltpu.VMEM((outer, rows, cols), low) for _ in range(3) for cols in both]
        + [pltpu.VMEM((seq_len, out_cols), low), pltpu.VMEM((seq_len, in_cols), low)]
        + [pltpu.SemaphoreType.DMA((outer, 2, 4)) for _ in range(4)],
        compiler_params=pltpu.CompilerParams(
            collective_id=2, has_side_effects=True, vmem_limit_bytes=36 * 2**20
        ),
    )(target, attn_rows, out_all, mixed, projected, probs)


def local(dp_size, clean_latents, noise_latents, step_index, labels, class_shift, w_qkv, w_out_t):
    latent_count, part_len, model_width = clean_latents.shape
    score_scale = 1.0 / math.sqrt(HEAD_DIM)
    seq_len = part_len * 4
    loss_scale = 1.0 / math.sqrt(dp_size * latent_count * seq_len)
    step_times, amplitude, amp_rate = time_terms(step_index, model_width)
    offset = lax.dynamic_slice(class_shift, (labels[0], 0), (1, model_width)).astype(jnp.float32)
    cos_t, sin_t = jnp.cos(step_times[0]), jnp.sin(step_times[0])
    row = (1, model_width)
    aux = jnp.concatenate(
        [
            1.0 + amplitude,
            amp_rate,
            offset,
            jnp.broadcast_to(cos_t, row),
            jnp.broadcast_to(sin_t, row),
            jnp.zeros((3, model_width), jnp.float32),
        ]
    )
    clean, noise = clean_latents[0], noise_latents[0]
    mixed_rows, _, _, out_all, projected, probs, attn_rows, blend = gather_all(
        dp_size, score_scale, clean, noise, aux, w_qkv, w_out_t
    )
    partial = lax.dot_general(
        blend, out_all, (((1,), (1,)), ((), ())), preferred_element_type=jnp.float32
    ).astype(jnp.bfloat16)
    target = gather_target(clean, noise, aux, partial)
    return back_all(
        dp_size, loss_scale, score_scale, target, attn_rows, out_all, mixed_rows, projected, probs
    )


def solution(mesh):
    in_specs = (
        P("dp", "tensor", None),
        P("dp", "tensor", None),
        P("dp"),
        P("dp"),
        P(),
        P("dp", "tensor"),
        P("dp", "tensor"),
    )
    out_specs = (P("dp", "tensor"), P("dp", "tensor"))
    step = functools.partial(local, mesh.shape["dp"])
    return jax.shard_map(step, mesh=mesh, in_specs=in_specs, out_specs=out_specs, check_vma=False)
```
